32 devices in a mesh: row: 8 (over z, x), gz: 4 (over y, core).
Axes of the slice: x: 2, y: 2, z: 4, core: 2. Of those that a mesh axis runs over, the one named last changes fastest.
Arguments:
- state: float32 [4, 1024, 16, 2048], P(None, 'row', 'gz'), may hold values from -12 to 12, as said below
- green: bfloat16 [8, 1024, 1024], P('row'), may hold values from -1 to 5
- vertical: float32 [16, 16], replicated, may hold values from 0 to 1
Outputs:
- new_state: float32 [4, 1024, 16, 2048], P(None, 'row', 'gz')
- potential: float32 [1024, 16, 2048], P('row', 'gz')
The draws below stay inside these ranges and needn't reach their ends.
Inputs may be any that keep to these rules, and one draw needn't show every extreme that they name: `state`: component 0 lies in 0.25 to 4; components 1 and 2 are at most 3 times component 0 in magnitude; component 3 lies between 0 and component 0.
All inputs are finite; a program needn't handle non-finite values.
Results may differ from the reference program's by a relative error of at most 0.0019.
Values may be sent and summed in bfloat16 or wider, within the bound.
No kernel may reach another device: no remote copies, remote signals or barrier semaphores. Data moves between devices by JAX's collectives and lax.ppermute only.
A program may use at most 192 MiB of HBM per device.

```python
import math
import jax
import jax.numpy as jnp
from jax import lax

NR = 1024
NPHI = 2048
MODES = 8
ZW = 16


def draw_state(key, part):
    keys = jax.random.split(jax.random.fold_in(key, 11), 4)
    shape = (NR, ZW, NPHI)
    level = jax.random.uniform(keys[0], shape, jnp.float32)
    density = 0.5 * 4.0 ** level
    radial_speed = 0.5 * jnp.clip(jax.random.normal(keys[1], shape, jnp.float32), -3.0, 3.0)
    spin_speed = 1.0 + 0.5 * jnp.clip(jax.random.normal(keys[2], shape, jnp.float32), -3.0, 3.0)
    tracer = jax.random.uniform(keys[3], shape, jnp.float32)
    return jnp.stack([density, density * radial_speed, density * spin_speed, density * tracer]).astype(jnp.float32)


def draw_green(key, part):
    base = jax.random.fold_in(key, 23)
    index = jnp.arange(NR)
    distance = jnp.abs(index[:, None] - index[None, :]).astype(jnp.float32)
    reach = NR / 4.0

    def one_mode(mode):
        keys = jax.random.split(jax.random.fold_in(base, mode), 3)
        strength = 0.5 * 4.0 ** jax.random.uniform(keys[0], (), jnp.float32)
        smooth = jnp.exp(-distance / reach) * (4.0 / NR) * strength
        rough = 0.5 * jnp.clip(jax.random.normal(keys[1], (NR, NR), jnp.float32), -4.0, 4.0) / math.sqrt(NR)
        diagonal = 1.0 + jax.random.uniform(keys[2], (NR,), jnp.float32)
        return (jnp.diag(diagonal) + rough + smooth).astype(jnp.bfloat16)
    return lax.map(one_mode, jnp.arange(MODES))


def draw_vertical(key, part):
    width = ZW / 4.0
    index = jnp.arange(ZW).astype(jnp.float32)
    offset = index[:, None] - index[None, :]
    shape_factor = jnp.exp(-offset * offset / (2.0 * width * width)) / (width * math.sqrt(2.0 * math.pi))
    noise = jnp.clip(jax.random.normal(jax.random.fold_in(key, 37), (ZW, ZW), jnp.float32), -3.0, 3.0)
    return (shape_factor * (1.0 + 0.3 * noise)).astype(jnp.float32)


def setup_inputs(seed: int = 0) -> dict:
    seeds = jax.random.split(jax.random.key(seed), 4)
    return {
        "state": draw_state(jax.random.fold_in(seeds[3], 71), 0),
        "green": draw_green(jax.random.fold_in(seeds[3], 71), 0),
        "vertical": draw_vertical(jax.random.fold_in(seeds[3], 71), 0),
    }


sound_sq = 1.0
inner_radius = 1.0
radial_span = 4.0
courant = 0.2
precise = lax.Precision.HIGHEST

def mode_table(azimuth, modes):
    angle_index = jnp.arange(azimuth, dtype=jnp.int32)[:, None] * jnp.arange(modes, dtype=jnp.int32)[None, :] % azimuth
    angles = angle_index.astype(jnp.float32) * (2.0 * math.pi / azimuth)
    forward = jnp.concatenate([jnp.cos(angles), -jnp.sin(angles)], axis=1)
    weights = jnp.where(jnp.arange(modes) == 0, 1.0, 2.0) / azimuth
    weights = jnp.concatenate([weights, weights]).astype(jnp.float32)
    inverse = forward.T * weights[:, None]
    return (forward, inverse)

def minmod(former, latter):
    return jnp.where(former * latter > 0, jnp.where(jnp.abs(former) < jnp.abs(latter), former, latter), 0.0)

def rusanov(left_state, right_state, normal):
    onehot = (jnp.arange(4) == normal).astype(left_state.dtype).reshape(4, 1, 1, 1)

    def flux_of(values):
        velocity = values[normal] / values[0]
        return (values * velocity + sound_sq * values[0] * onehot, jnp.abs(velocity))
    flux_left, speed_left = flux_of(left_state)
    flux_right, speed_right = flux_of(right_state)
    reach = jnp.maximum(speed_left, speed_right) + math.sqrt(sound_sq)
    return 0.5 * (flux_left + flux_right) - 0.5 * reach * (right_state - left_state)

def advance(padded, potential, radial_slope, centres, radial_step):
    azimuth = padded.shape[-1]
    phi_step = 2.0 * math.pi / azimuth
    step_time = courant * min(radial_step, inner_radius * phi_step)
    slopes = minmod(padded[:, 1:-1] - padded[:, :-2], padded[:, 2:] - padded[:, 1:-1])
    centre_cells = padded[:, 1:-1]
    flux_radial = rusanov(centre_cells[:, :-1] + 0.5 * slopes[:, :-1], centre_cells[:, 1:] - 0.5 * slopes[:, 1:], 1)
    interior = padded[:, 2:-2]
    phi_slopes = minmod(interior - jnp.roll(interior, 1, axis=3), jnp.roll(interior, -1, axis=3) - interior)
    flux_phi = rusanov(interior + 0.5 * phi_slopes, jnp.roll(interior - 0.5 * phi_slopes, -1, axis=3), 2)
    face_radii = jnp.concatenate([centres - 0.5 * radial_step, centres[-1:] + 0.5 * radial_step]).reshape(1, -1, 1, 1)
    weighted = face_radii * flux_radial
    radius = centres.reshape(1, -1, 1, 1)
    tendency = -((weighted[:, 1:] - weighted[:, :-1]) / radial_step + (flux_phi - jnp.roll(flux_phi, 1, axis=3)) / phi_step) / radius
    density = interior[0]
    spin = interior[2] / density
    radius_cells = centres.reshape(-1, 1, 1)
    azimuth_slope = (jnp.roll(potential, -1, axis=2) - jnp.roll(potential, 1, axis=2)) / (2.0 * phi_step)
    force_radial = (interior[2] * spin + sound_sq * density) / radius_cells - density * radial_slope
    force_phi = -(interior[1] * spin + density * azimuth_slope) / radius_cells
    zeros = jnp.zeros_like(density)
    sources = jnp.stack([zeros, force_radial, force_phi, zeros])
    return interior + step_time * (tendency + sources)

def reference(state, green, vertical):
    forward, inverse = mode_table(NPHI, MODES)
    spectrum = jnp.dot(state[0].reshape(-1, NPHI), forward, precision=precise, preferred_element_type=jnp.float32).reshape(NR, ZW, 2, MODES)
    mixed = jnp.einsum('zy,ryck->rzck', vertical, spectrum, precision=precise)
    mixed_b = mixed.astype(jnp.bfloat16)

    def one_mode(operands):
        matrix, column = operands
        return jnp.einsum('rs,szc->rzc', matrix.astype(jnp.float32), column.astype(jnp.float32))
    mode_major = lax.map(one_mode, (green, jnp.moveaxis(mixed_b, 3, 0)))
    pot_spec = jnp.moveaxis(mode_major, 0, 3)
    potential = jnp.dot(pot_spec.reshape(-1, 2 * MODES), inverse, precision=precise, preferred_element_type=jnp.float32).reshape(NR, ZW, NPHI)
    radial_step = radial_span / NR
    padded_pot = jnp.pad(potential, ((1, 1), (0, 0), (0, 0)), mode='edge')
    radial_slope = (padded_pot[2:] - padded_pot[:-2]) / (2.0 * radial_step)
    padded = jnp.pad(state, ((0, 0), (2, 2), (0, 0), (0, 0)), mode='edge')
    centres = inner_radius + (jnp.arange(NR).astype(jnp.float32) + 0.5) * radial_step
    new_state = advance(padded, potential, radial_slope, centres, radial_step)
    return (new_state, potential)
```

```python
import math

import jax
import jax.numpy as jnp
import numpy as np
from jax import lax
from jax.experimental import pallas as pl
from jax.experimental.pallas import tpu as pltpu
from jax.sharding import PartitionSpec as P

sound_sq = 1.0
inner_radius = 1.0
radial_span = 4.0
courant = 0.2
precise = lax.Precision.HIGHEST


def padded_2(cells, sides, width):
    for axis, dim in sides:
        count = lax.axis_size(axis)
        ends = count - 1
        head = lax.slice_in_dim(cells, 0, width, axis=dim)
        tail = lax.slice_in_dim(cells, cells.shape[dim] - width, cells.shape[dim], axis=dim)
        cells = jnp.concatenate(
            [
                lax.ppermute(tail, axis, [(i, (i + 1) % count) for i in range(ends)]),
                cells,
                lax.ppermute(head, axis, [((i + 1) % count, i) for i in range(ends)]),
            ],
            axis=dim,
        )
    return cells


def mode_table(azimuth, modes):
    angle_index = (
        jnp.arange(azimuth, dtype=jnp.int32)[:, None]
        * jnp.arange(modes, dtype=jnp.int32)[None, :]
        % azimuth
    )
    angles = angle_index.astype(jnp.float32) * (2.0 * math.pi / azimuth)
    forward = jnp.concatenate([jnp.cos(angles), -jnp.sin(angles)], axis=1)
    weights = jnp.where(jnp.arange(modes) == 0, 1.0, 2.0) / azimuth
    weights = jnp.concatenate([weights, weights]).astype(jnp.float32)
    inverse = forward.T * weights[:, None]
    return (forward, inverse)


def minmod(former, latter):
    return jnp.where(
        former * latter > 0, jnp.where(jnp.abs(former) < jnp.abs(latter), former, latter), 0.0
    )


def rusanov(left_state, right_state, normal):
    onehot = (jnp.arange(4) == normal).astype(left_state.dtype).reshape(4, 1, 1, 1)

    def flux_of(values):
        velocity = values[normal] / values[0]
        return (values * velocity + sound_sq * values[0] * onehot, jnp.abs(velocity))

    flux_left, speed_left = flux_of(left_state)
    flux_right, speed_right = flux_of(right_state)
    reach = jnp.maximum(speed_left, speed_right) + math.sqrt(sound_sq)
    return 0.5 * (flux_left + flux_right) - 0.5 * reach * (right_state - left_state)


def advance(padded, potential, radial_slope, centres, radial_step):
    azimuth = padded.shape[-1]
    phi_step = 2.0 * math.pi / azimuth
    step_time = courant * min(radial_step, inner_radius * phi_step)
    slopes = minmod(padded[:, 1:-1] - padded[:, :-2], padded[:, 2:] - padded[:, 1:-1])
    centre_cells = padded[:, 1:-1]
    flux_radial = rusanov(
        centre_cells[:, :-1] + 0.5 * slopes[:, :-1], centre_cells[:, 1:] - 0.5 * slopes[:, 1:], 1
    )
    interior = padded[:, 2:-2]
    phi_slopes = minmod(
        interior - jnp.roll(interior, 1, axis=3), jnp.roll(interior, -1, axis=3) - interior
    )
    flux_phi = rusanov(
        interior + 0.5 * phi_slopes, jnp.roll(interior - 0.5 * phi_slopes, -1, axis=3), 2
    )
    face_radii = jnp.concatenate(
        [centres - 0.5 * radial_step, centres[-1:] + 0.5 * radial_step]
    ).reshape(1, -1, 1, 1)
    weighted = face_radii * flux_radial
    radius = centres.reshape(1, -1, 1, 1)
    tendency = (
        -(
            (weighted[:, 1:] - weighted[:, :-1]) / radial_step
            + (flux_phi - jnp.roll(flux_phi, 1, axis=3)) / phi_step
        )
        / radius
    )
    density = interior[0]
    spin = interior[2] / density
    radius_cells = centres.reshape(-1, 1, 1)
    azimuth_slope = (jnp.roll(potential, -1, axis=2) - jnp.roll(potential, 1, axis=2)) / (
        2.0 * phi_step
    )
    force_radial = (interior[2] * spin + sound_sq * density) / radius_cells - density * radial_slope
    force_phi = -(interior[1] * spin + density * azimuth_slope) / radius_cells
    zeros = jnp.zeros_like(density)
    sources = jnp.stack([zeros, force_radial, force_phi, zeros])
    return interior + step_time * (tendency + sources)


def mend_edges(padded, width, axis_dim):
    length = padded.shape[axis_dim]
    position = lax.axis_index("row")
    last_rank = lax.axis_size("row") - 1
    low_rim = lax.slice_in_dim(padded, 0, width, axis=axis_dim)
    middle = lax.slice_in_dim(padded, width, length - width, axis=axis_dim)
    high_rim = lax.slice_in_dim(padded, length - width, length, axis=axis_dim)
    first_cell = lax.slice_in_dim(middle, 0, 1, axis=axis_dim)
    last_cell = lax.slice_in_dim(
        middle, middle.shape[axis_dim] - 1, middle.shape[axis_dim], axis=axis_dim
    )
    low_rim = jnp.where(position == 0, jnp.broadcast_to(first_cell, low_rim.shape), low_rim)
    high_rim = jnp.where(
        position == last_rank, jnp.broadcast_to(last_cell, high_rim.shape), high_rim
    )
    return jnp.concatenate([low_rim, middle, high_rim], axis=axis_dim)


def plain_body(state, green, vertical):
    radii, planes, azimuth = (state.shape[1], state.shape[2], state.shape[3])
    modes_dev, radial_all = (green.shape[0], green.shape[1])
    modes = modes_dev * lax.axis_size("row")
    radial_step = radial_span / radial_all
    forward, inverse = mode_table(azimuth, modes)
    padded_state = mend_edges(padded_2(state, (("row", 1),), 2), 2, 1)
    spectrum = jnp.dot(
        state[0].reshape(-1, azimuth),
        forward,
        precision=precise,
        preferred_element_type=jnp.float32,
    ).reshape(radii, planes, 2, modes)
    plane_start = lax.axis_index("gz") * planes
    column_all = lax.all_gather(spectrum, "gz", axis=1, tiled=True)
    own_rows = lax.dynamic_slice_in_dim(vertical, plane_start, planes, 0)
    mixed = jnp.einsum("zy,ryck->rzck", own_rows, column_all, precision=precise)
    mixed_b = mixed.astype(jnp.bfloat16)
    pot_modes = jnp.einsum(
        "mrs,skcm->rkcm",
        green,
        lax.all_to_all(mixed_b, "row", split_axis=3, concat_axis=0, tiled=True),
        preferred_element_type=jnp.float32,
    )
    pot_spec = lax.all_to_all(pot_modes, "row", split_axis=0, concat_axis=3, tiled=True)
    potential = jnp.dot(
        pot_spec.reshape(-1, 2 * modes),
        inverse,
        precision=precise,
        preferred_element_type=jnp.float32,
    ).reshape(radii, planes, azimuth)
    padded_pot = mend_edges(padded_2(potential, (("row", 0),), 1), 1, 0)
    radial_slope = (padded_pot[2:] - padded_pot[:-2]) / (2.0 * radial_step)
    offsets = (lax.axis_index("row") * radii + jnp.arange(radii, dtype=jnp.int32)).astype(
        jnp.float32
    )
    centres = inner_radius + (offsets + 0.5) * radial_step
    new_state = advance(padded_state, potential, radial_slope, centres, radial_step)
    return (new_state, potential)


LANES = 128
SUBS = 8
HALF = 4
PAIRS = ((0, 0), (0, 1), (1, 0), (0, 2), (2, 0), (1, 1))


def np_split3(values):
    high = np.asarray(values, np.float32)
    parts = []
    for _ in range(3):
        part = high.astype(jnp.bfloat16)
        parts.append(part)
        high = high - part.astype(np.float32)
    return parts


def np_tables(azimuth, modes):
    index = np.arange(azimuth)[:, None] * np.arange(modes)[None, :] % azimuth
    angles = index * (2.0 * np.pi / azimuth)
    forward = np.concatenate([np.cos(angles), -np.sin(angles)], axis=1)
    weights = np.where(np.arange(modes) == 0, 1.0, 2.0) / azimuth
    inverse = forward.T * np.concatenate([weights, weights])[:, None]
    phi_step = 2.0 * np.pi / azimuth
    turned = (np.roll(inverse, -1, 1) - np.roll(inverse, 1, 1)) / (2.0 * phi_step)
    return (forward, inverse, turned)


def forward_table(forward):
    azimuth, width = forward.shape
    tiles = azimuth // (2 * LANES)
    table = np.zeros((tiles, LANES, 2, HALF, width), jnp.bfloat16)
    blocks = forward.reshape(tiles, 2, LANES, width)
    for q, part in enumerate(np_split3(blocks)):
        table[:, :, :, q] = part.transpose(0, 2, 1, 3)
    return table.reshape(tiles * LANES, 2 * HALF * width)


def inverse_table(inverse):
    width, azimuth = inverse.shape
    tiles = azimuth // (2 * LANES)
    parts = np_split3(inverse.reshape(width, tiles, 2, LANES))
    table = np.zeros((2, LANES // width, width, tiles, LANES), jnp.bfloat16)
    for q, (_, right) in enumerate(PAIRS):
        table[:, q] = parts[right].transpose(2, 0, 1, 3)
    return table.reshape(2 * LANES, tiles * LANES)


def split3(values):
    parts = []
    for _ in range(3):
        part = values.astype(jnp.bfloat16)
        parts.append(part)
        values = values - part.astype(jnp.float32)
    return parts


def lane_of(shape):
    return lax.broadcasted_iota(jnp.int32, shape, len(shape) - 1)


def spectrum_kernel(copies, cells_ref, table_ref, out_ref, sums_ref):
    step = pl.program_id(0)
    rows, _, _ = cells_ref.shape[1:]
    tiles = cells_ref.shape[2] // SUBS
    total = None
    for t in range(0, tiles, 2):
        cells = jnp.concatenate(
            [
                cells_ref[0, :, (t + h) * SUBS : (t + h + 1) * SUBS, :].reshape(rows * SUBS, LANES)
                for h in range(2)
            ],
            axis=1,
        )
        table = table_ref[t * LANES : (t + 2) * LANES, :]
        for part in split3(cells):
            term = jnp.dot(part, table, preferred_element_type=jnp.float32)
            total = term if total is None else total + term
    sums_ref[pl.ds(pl.multiple_of(step * rows * SUBS, SUBS), rows * SUBS), :] = total

    @pl.when(step == pl.num_programs(0) - 1)
    def _():
        radii = sums_ref.shape[0] // SUBS
        modes = out_ref.shape[0]
        width = 2 * modes
        lane = lane_of((radii, LANES))
        for z in range(HALF):
            former = sums_ref[pl.ds(z, radii, stride=SUBS), :]
            latter = sums_ref[pl.ds(HALF + z, radii, stride=SUBS), :]
            turned = jnp.where(lane < LANES // 2, former, latter).T
            both = turned[: LANES // 2] + turned[LANES // 2 :]
            value = both[:width] + both[width : 2 * width] + both[2 * width : 3 * width]
            for c in range(2):
                for g in range(copies):
                    out_ref[:, g, c * HALF + z, :] = value[c * modes : (c + 1) * modes]


def green_kernel(cells_ref, weights_ref, green_ref, out_ref):
    blocks = cells_ref.shape[0]
    mixed = [
        jnp.dot(
            weights_ref[...],
            cells_ref[i],
            precision=precise,
            preferred_element_type=jnp.float32,
        )
        for i in range(blocks)
    ]
    mixed = jnp.concatenate(mixed, axis=1).astype(jnp.bfloat16)
    pot = lax.dot_general(
        mixed, green_ref[0], (((1,), (1,)), ((), ())), preferred_element_type=jnp.float32
    )
    lane = lane_of((SUBS, LANES))
    pieces = [pot[:, i * LANES : (i + 1) * LANES] for i in range(blocks)]
    for i in range(blocks):
        out_ref[i, 0] = pieces[i]
        low = pieces[0] if i == 0 else pltpu.roll(pieces[i - 1], 1, 1)
        if i == blocks - 1:
            high = pltpu.roll(pieces[i], 2, 1)
        else:
            high = pltpu.roll(pieces[i + 1], 1, 1)
        out_ref[i, 1] = jnp.where(lane == 0, low, high)


def limited(former, latter):
    return jnp.maximum(jnp.minimum(former, latter), jnp.minimum(jnp.maximum(former, latter), 0.0))


def face_flux(left, right, normal):
    inverse = 1.0 / (left[0] * right[0])
    speed_left = left[normal] * (right[0] * inverse)
    speed_right = right[normal] * (left[0] * inverse)
    reach = jnp.maximum(jnp.abs(speed_left), jnp.abs(speed_right)) + math.sqrt(sound_sq)
    weight_left = speed_left + reach
    weight_right = speed_right - reach
    fluxes = [a * weight_left + b * weight_right for a, b in zip(left, right)]
    fluxes[normal] = fluxes[normal] + sound_sq * (left[0] + right[0])
    return fluxes


def block_step(cell, base_row, constants, scratch, store, pull, fresh):
    rows, subs, radial_step, phi_step, step_time = constants
    d_ref, r_ref, g_ref, w_ref, l_ref, f_ref = scratch
    tiles = subs // SUBS
    lane = lane_of((SUBS, LANES))
    first = lane == 0
    last = lane == LANES - 1

    def up(here, there):
        return pltpu.roll(jnp.where(first, there, here), LANES - 1, 1)

    def down(here, there):
        return pltpu.roll(jnp.where(last, there, here), 1, 1)

    def span(k, shift):
        return pl.ds(k * SUBS + SUBS + shift, SUBS)

    def radial_face(r, k):
        part = pl.ds(k * SUBS, SUBS)
        left, right = [], []
        for f in range(4):
            here, above, far = cell(f, r, k), cell(f, r + 1, k), cell(f, r + 2, k)
            slope = limited(above - here, far - above)
            twice = above + above
            left.append(l_ref[f, part, :])
            right.append(twice - slope)
            l_ref[f, part, :] = twice + slope
        return face_flux(left, right, 1)

    @pl.when(fresh)
    def _():
        for k in range(tiles):
            part = pl.ds(k * SUBS, SUBS)
            for f in range(4):
                lower, here, above = cell(f, -2, k), cell(f, -1, k), cell(f, 0, k)
                l_ref[f, part, :] = (here + here) + limited(here - lower, above - here)
            for f, value in enumerate(radial_face(-1, k)):
                f_ref[f, part, :] = value

    for r in range(rows):
        slot = r % 2
        index = (base_row + r).astype(jnp.float32)
        centre = inner_radius + (jnp.full((SUBS, LANES), index, jnp.float32) + 0.5) * radial_step
        over = step_time / centre
        scale = over * (0.25 / radial_step)
        outer = scale * (centre + 0.5 * radial_step)
        inner = scale * (centre - 0.5 * radial_step)
        turn = over * (0.25 / phi_step)
        for k in range(tiles):
            for f in range(4):
                here = cell(f, r, k)
                if k + 1 < tiles:
                    there = cell(f, r, k, HALF)
                else:
                    there = jnp.concatenate(
                        [cell(f, r, k)[HALF:], cell(f, r, 0)[:HALF]], axis=0
                    )
                delta = up(here, there) - here
                d_ref[slot, f, span(k, 0), :] = delta
                if k == tiles - 1:
                    d_ref[slot, f, HALF:SUBS, :] = delta[HALF:]
        for k in range(tiles):
            for f in range(4):
                here = cell(f, r, k)
                ahead = d_ref[slot, f, span(k, 0), :]
                behind = down(ahead, d_ref[slot, f, span(k, -HALF), :])
                slope = limited(behind, ahead)
                twice = here + here
                w_ref[slot, f, span(k, 0), :] = twice + slope
                right = twice - slope
                r_ref[slot, f, span(k, 0), :] = right
                if k == 0:
                    r_ref[slot, f, pl.ds(SUBS + subs, HALF), :] = right[:HALF]
        for k in range(tiles):
            left = [w_ref[slot, f, span(k, 0), :] for f in range(4)]
            right = [
                up(r_ref[slot, f, span(k, 0), :], r_ref[slot, f, span(k, HALF), :])
                for f in range(4)
            ]
            for f, value in enumerate(face_flux(left, right, 2)):
                g_ref[slot, f, span(k, 0), :] = value
                if k == tiles - 1:
                    g_ref[slot, f, HALF:SUBS, :] = value[HALF:]
        for k in range(tiles):
            part = pl.ds(k * SUBS, SUBS)
            radial = radial_face(r, k)
            values = [cell(f, r, k) for f in range(4)]
            density, push, swing, _ = values
            spin = swing / density
            extra = [None, (swing * spin + sound_sq * density) * over, (push * spin) * -over, None]
            for f, value in enumerate(values):
                flux = g_ref[slot, f, span(k, 0), :]
                before = down(flux, g_ref[slot, f, span(k, -HALF), :])
                value = value + (inner * f_ref[f, part, :] - outer * radial[f])
                value = value - turn * (flux - before)
                if extra[f] is not None:
                    value = value + extra[f]
                    if pull is not None:
                        value = value - density * pull(f - 1, r, k)
                f_ref[f, part, :] = radial[f]
                store(f, r, k, value)


def spectral_rows(modes_ref, left_ref, radial_step, step_time):
    modes = modes_ref.shape[0]
    width = 2 * modes
    radii = LANES
    lane = lane_of((modes, LANES))
    index = (lane + lax.axis_index("row") * radii).astype(jnp.float32)
    over = step_time / (inner_radius + (index + 0.5) * radial_step)
    left_ref[...] = jnp.zeros_like(left_ref)
    for z in range(HALF):
        kinds = ([], [], [])
        for c in range(2):
            here = modes_ref[:, 0, c * HALF + z, :]
            edge = modes_ref[:, 1, c * HALF + z, :]
            above = jnp.where(
                lane == LANES - 1, pltpu.roll(edge, LANES - 2, 1), pltpu.roll(here, LANES - 1, 1)
            )
            below = jnp.where(lane == 0, edge, pltpu.roll(here, 1, 1))
            kinds[0].append(here)
            kinds[1].append((above - below) * (step_time / (2.0 * radial_step)))
            kinds[2].append(here * over)
        for kind, halves in enumerate(kinds):
            parts = [part.astype(jnp.float32) for part in split3(jnp.concatenate(halves, axis=0))]
            stack = [parts[left] for left, _ in PAIRS]
            stack += [jnp.zeros((LANES - len(PAIRS) * width, LANES), jnp.float32)]
            turned = jnp.concatenate(stack, axis=0).T
            for p in range(2):
                left_ref[kind, p, pl.ds(p * HALF + z, radii, stride=SUBS), :] = turned


def muscl_kernel(plan, final, *refs):
    rows, subs, radii, radial_all, start, count, done = plan
    if final:
        cells, low, high, modes_ref, pot_table, turn_table, old, out, pot_out, *refs = refs
        left_ref, pull_ref, pot_buf, late_buf, pot_sem, late_sem, *refs = refs
    else:
        cells, out, *refs = refs
    in_buf, out_buf, in_sem, out_sem, *scratch = refs
    azimuth = subs // HALF * LANES
    phi_step = 2.0 * math.pi / azimuth
    radial_step = radial_span / radial_all
    step_time = courant * min(radial_step, inner_radius * phi_step)
    blocks = radii // rows
    size = rows * subs
    full = (rows + 4) * subs
    position = lax.axis_index("row")
    last_rank = lax.axis_size("row") - 1
    tiles = subs // SUBS

    def place(n):
        return lax.rem(start + n, blocks)

    def copy_in(source, f, first, length, slot, offset):
        return pltpu.make_async_copy(
            source.at[f, pl.ds(first, length), :],
            in_buf.at[slot, f, pl.ds(offset, length), :],
            in_sem.at[slot],
        )

    def fetch(n, slot):
        b = place(n)
        base = pl.multiple_of(b * size, size)
        inside = (b > 0) & (b < blocks - 1)

        @pl.when(inside)
        def _():
            for f in range(4):
                copy_in(cells, f, base - 2 * subs, full, slot, 0).start()

        if not final:
            return

        @pl.when(b == 0)
        def _():
            for f in range(4):
                copy_in(cells, f, 0, size + 2 * subs, slot, 2 * subs).start()

            @pl.when(position == 0)
            def _():
                for f in range(4):
                    for h in range(2):
                        copy_in(cells, f, 0, subs, slot, h * subs).start()

            @pl.when(position != 0)
            def _():
                for f in range(4):
                    copy_in(low, f, 0, 2 * subs, slot, 0).start()

        @pl.when(b == blocks - 1)
        def _():
            for f in range(4):
                copy_in(cells, f, (radii - rows - 2) * subs, size + 2 * subs, slot, 0).start()

            @pl.when(position == last_rank)
            def _():
                for f in range(4):
                    for h in range(2):
                        copy_in(
                            cells, f, (radii - 1) * subs, subs, slot, size + (2 + h) * subs
                        ).start()

            @pl.when(position != last_rank)
            def _():
                for f in range(4):
                    copy_in(high, f, 0, 2 * subs, slot, size + 2 * subs).start()

    def arrived(slot):
        for f in range(4):
            copy_in(cells, f, 0, full, slot, 0).wait()

    def give(n, slot):
        base = pl.multiple_of(place(n) * size, size)
        copies = [
            pltpu.make_async_copy(
                out_buf.at[slot, f, pl.ds(0, size), :],
                out.at[f, pl.ds(base, size), :],
                out_sem.at[slot],
            )
            for f in range(4)
        ]
        if final:
            copies.append(
                pltpu.make_async_copy(
                    pot_buf.at[slot], pot_out.at[pl.ds(base, size), :], out_sem.at[slot]
                )
            )
        return copies

    fetch(0, 0)
    if final:
        spectral_rows(modes_ref, left_ref, radial_step, step_time)

    def spectral(b, pot_slot):
        span = pl.ds(pl.multiple_of(b * rows * SUBS, SUBS), rows * SUBS)

        def product(kinds, table):
            left = [
                jnp.concatenate([left_ref[kind, p, span, :] for p in range(2)], axis=1)
                for kind in kinds
            ]
            left = jnp.concatenate(left, axis=0).astype(jnp.bfloat16)
            return jnp.dot(left, table[...], preferred_element_type=jnp.float32)

        both = product((0, 1), pot_table)
        turn = product((2,), turn_table)
        for r in range(rows):
            for t in range(tiles):
                part = pl.ds(r * subs + t * SUBS, SUBS)
                column = slice(t * LANES, (t + 1) * LANES)
                line = slice(r * SUBS, (r + 1) * SUBS)
                pot_buf[pot_slot, part, :] = both[line, column]
                pull_ref[0, part, :] = both[rows * SUBS + r * SUBS : rows * SUBS + (r + 1) * SUBS, column]
                pull_ref[1, part, :] = turn[line, column]

    def body(n, carry):
        slot = lax.rem(n, 2)

        @pl.when(n + 1 < count)
        def _():
            fetch(n + 1, 1 - slot)

        @pl.when(n >= 2)
        def _():
            for copy in give(n - 2, slot):
                copy.wait()

        b = place(n)
        pull = None
        if final:
            spectral(b, slot)

            def pull(kind, r, k):
                return pull_ref[kind, pl.ds(r * subs + k * SUBS, SUBS), :]

        arrived(slot)

        def cell(f, r, k, shift=0):
            return in_buf[slot, f, pl.ds((r + 2) * subs + k * SUBS + shift, SUBS), :]

        def store(f, r, k, value):
            out_buf[slot, f, pl.ds(r * subs + k * SUBS, SUBS), :] = value

        constants = (rows, subs, radial_step, phi_step, step_time)
        block_step(
            cell, position * radii + b * rows, constants, scratch, store, pull, (n == 0) | (b == 0)
        )
        for copy in give(n, slot):
            copy.start()
        return carry

    lax.fori_loop(0, count, body, 0)
    for n in range(max(count - 2, 0), count):
        for copy in give(n, n % 2):
            copy.wait()
    if not final:
        return

    def late_in(n, slot):
        base = pl.multiple_of((1 + n) * size, size)
        return [
            pltpu.make_async_copy(
                source.at[f, pl.ds(base, size), :], late_buf.at[slot, i], late_sem.at[slot]
            )
            for i, (source, f) in enumerate(((cells, 0), (out, 1), (out, 2)))
        ]

    def late_out(n, slot):
        base = pl.multiple_of((1 + n) * size, size)
        copies = [
            pltpu.make_async_copy(
                out_buf.at[slot, f, pl.ds(0, size), :],
                out.at[f, pl.ds(base, size), :],
                pot_sem.at[slot],
            )
            for f in (1, 2)
        ]
        copies.append(
            pltpu.make_async_copy(
                pot_buf.at[slot], pot_out.at[pl.ds(base, size), :], pot_sem.at[slot]
            )
        )
        return copies

    for copy in late_in(0, 0):
        copy.start()

    def late(n, carry):
        slot = lax.rem(n, 2)

        @pl.when(n + 1 < done)
        def _():
            for copy in late_in(n + 1, 1 - slot):
                copy.start()

        @pl.when(n >= 2)
        def _():
            for copy in late_out(n - 2, slot):
                copy.wait()

        spectral(1 + n, slot)
        for copy in late_in(n, slot):
            copy.wait()
        for t in range(rows * tiles):
            part = pl.ds(t * SUBS, SUBS)
            density = late_buf[slot, 0, part, :]
            for f in (1, 2):
                out_buf[slot, f, part, :] = (
                    late_buf[slot, f, part, :] - density * pull_ref[f - 1, part, :]
                )
        for copy in late_out(n, slot):
            copy.start()
        return carry

    lax.fori_loop(0, done, late, 0)
    for n in range(max(done - 2, 0), done):
        for copy in late_out(n, n % 2):
            copy.wait()


def vmem_limit(mebibytes):
    return pltpu.CompilerParams(vmem_limit_bytes=mebibytes * 2**20)


def muscl(operands, plan, final, shape):
    rows, subs, radii, _, _, count, _ = plan
    fields = shape[0]
    size = rows * subs
    pad = subs + 3 * SUBS
    anywhere = pl.BlockSpec(memory_space=pl.ANY)
    whole = pl.BlockSpec(memory_space=pltpu.VMEM)
    carried = [
        pltpu.VMEM((2, fields, (rows + 4) * subs + SUBS, LANES), jnp.float32),
        pltpu.VMEM((2, fields, size + SUBS, LANES), jnp.float32),
        pltpu.SemaphoreType.DMA((2,)),
        pltpu.SemaphoreType.DMA((2,)),
    ]
    carried += [pltpu.VMEM((2, fields, pad, LANES), jnp.float32) for _ in range(4)]
    carried += [pltpu.VMEM((fields, subs + SUBS, LANES), jnp.float32) for _ in range(2)]
    out_shape = [jax.ShapeDtypeStruct(shape, jnp.float32)]
    if final:
        in_specs = [anywhere] * 3 + [whole] * 3 + [anywhere]
        out_shape.append(jax.ShapeDtypeStruct(shape[1:], jnp.float32))
        aliases = {6: 0}
        carried = [
            pltpu.VMEM((3, 2, radii * SUBS, LANES), jnp.float32),
            pltpu.VMEM((2, size, LANES), jnp.float32),
            pltpu.VMEM((2, size, LANES), jnp.float32),
            pltpu.VMEM((2, 3, size, LANES), jnp.float32),
            pltpu.SemaphoreType.DMA((2,)),
            pltpu.SemaphoreType.DMA((2,)),
        ] + carried
    else:
        in_specs = [anywhere]
        aliases = {}
    return pl.pallas_call(
        lambda *refs: muscl_kernel(plan, final, *refs),
        name="muscl_final" if final else "muscl_early",
        in_specs=in_specs,
        out_specs=[anywhere] * len(out_shape),
        out_shape=out_shape,
        input_output_aliases=aliases,
        scratch_shapes=carried,
        compiler_params=vmem_limit(50),
        cost_estimate=pl.CostEstimate(
            flops=count * rows * subs * LANES * 1500,
            bytes_accessed=count * size * LANES * 32,
            transcendentals=0,
        ),
    )(*operands)


def fast_body(state, green, vertical):
    fields, radii, planes, azimuth = state.shape
    radial_all = green.shape[1]
    ranks, stacks = lax.axis_size("row"), lax.axis_size("gz")
    modes = green.shape[0] * ranks
    subs = azimuth // LANES * planes
    forward, inverse, turned = np_tables(azimuth, modes)
    cells = (
        state.reshape(fields, radii, planes, azimuth // LANES, LANES)
        .transpose(0, 1, 3, 2, 4)
        .reshape(fields, radii, subs, LANES)
    )
    up_ring = [(i, i + 1) for i in range(ranks - 1)]
    low = lax.ppermute(cells[:, radii - 2 :], "row", up_ring)
    high = lax.ppermute(cells[:, :2], "row", [(j, i) for i, j in up_ring])

    rows = 16
    spectrum = pl.pallas_call(
        lambda *refs: spectrum_kernel(stacks, *refs),
        name="spectrum",
        grid=(radii // rows,),
        in_specs=[
            pl.BlockSpec((1, rows, subs, LANES), lambda i: (0, i, 0, 0)),
            pl.BlockSpec((azimuth // 2, LANES), lambda i: (0, 0)),
        ],
        out_specs=pl.BlockSpec((modes, stacks, SUBS, LANES), lambda i: (0, 0, 0, 0)),
        out_shape=jax.ShapeDtypeStruct((modes, stacks, SUBS, LANES), jnp.float32),
        scratch_shapes=[pltpu.VMEM((radii * SUBS, LANES), jnp.float32)],
        compiler_params=vmem_limit(54),
        cost_estimate=pl.CostEstimate(flops=2**33, bytes_accessed=2**22, transcendentals=0),
    )(cells, forward_table(forward))

    gathered = lax.all_to_all(
        spectrum.reshape(ranks * stacks, SUBS, LANES), ("row", "gz"), 0, 0, tiled=True
    )
    own = lax.dynamic_slice_in_dim(vertical, lax.axis_index("gz") * planes, planes, 0)
    own = own.reshape(planes, stacks, planes)
    weights = jnp.einsum("cd,zgy->czgdy", jnp.eye(2, dtype=jnp.float32), own, precision=precise)
    weights = weights.reshape(SUBS, stacks * SUBS)

    pot_modes = pl.pallas_call(
        green_kernel,
        name="green",
        in_specs=[pl.BlockSpec(memory_space=pltpu.VMEM)] * 3,
        out_specs=pl.BlockSpec(memory_space=pltpu.VMEM),
        out_shape=jax.ShapeDtypeStruct((ranks, 2, SUBS, LANES), jnp.float32),
        compiler_params=vmem_limit(16),
        cost_estimate=pl.CostEstimate(flops=2**30, bytes_accessed=2**21, transcendentals=0),
    )(gathered.reshape(ranks, stacks * SUBS, LANES), weights, green)
    pot_spec = lax.all_to_all(pot_modes, "row", 0, 0, tiled=True)

    rows, early = 8, 3
    blocks = radii // rows
    flat = cells.reshape(fields, radii * subs, LANES)
    flat_low = low.reshape(fields, 2 * subs, LANES)
    flat_high = high.reshape(fields, 2 * subs, LANES)
    plan = (rows, subs, radii, radial_all, 1, early, 0)
    (partial,) = muscl([flat], plan, False, flat.shape)
    plan = (rows, subs, radii, radial_all, 1 + early, blocks - early, early)
    new_cells, potential = muscl(
        [
            flat,
            flat_low,
            flat_high,
            pot_spec,
            inverse_table(inverse),
            inverse_table(turned),
            partial,
        ],
        plan,
        True,
        flat.shape,
    )
    new_state = (
        new_cells.reshape(fields, radii, azimuth // LANES, planes, LANES)
        .transpose(0, 1, 3, 2, 4)
        .reshape(state.shape)
    )
    potential = (
        potential.reshape(radii, azimuth // LANES, planes, LANES)
        .transpose(0, 2, 1, 3)
        .reshape(state.shape[1:])
    )
    return (new_state, potential)


def body(state, green, vertical):
    _, radii, planes, azimuth = state.shape
    modes = green.shape[0] * lax.axis_size("row")
    fits = (
        planes == HALF
        and azimuth % (4 * LANES) == 0
        and radii == LANES
        and green.shape[0] == 1
        and modes == SUBS
    )
    return (fast_body if fits else plain_body)(state, green, vertical)


def solution(mesh):
    placed = (P(None, "row", "gz", None), P("row", None, None), P())
    return jax.shard_map(
        body,
        mesh=mesh,
        in_specs=placed,
        out_specs=(P(None, "row", "gz", None), P("row", "gz", None)),
        check_vma=False,
    )
```

```python
import math

import jax
import jax.numpy as jnp
import numpy as np
from jax import lax
from jax.experimental import pallas as pl
from jax.experimental.pallas import tpu as pltpu
from jax.sharding import PartitionSpec as P

sound_sq = 1.0
inner_radius = 1.0
radial_span = 4.0
courant = 0.2
precise = lax.Precision.HIGHEST


def padded_2(cells, sides, width):
    for axis, dim in sides:
        count = lax.axis_size(axis)
        ends = count - 1
        head = lax.slice_in_dim(cells, 0, width, axis=dim)
        tail = lax.slice_in_dim(cells, cells.shape[dim] - width, cells.shape[dim], axis=dim)
        cells = jnp.concatenate(
            [
                lax.ppermute(tail, axis, [(i, (i + 1) % count) for i in range(ends)]),
                cells,
                lax.ppermute(head, axis, [((i + 1) % count, i) for i in range(ends)]),
            ],
            axis=dim,
        )
    return cells


def mode_table(azimuth, modes):
    angle_index = (
        jnp.arange(azimuth, dtype=jnp.int32)[:, None]
        * jnp.arange(modes, dtype=jnp.int32)[None, :]
        % azimuth
    )
    angles = angle_index.astype(jnp.float32) * (2.0 * math.pi / azimuth)
    forward = jnp.concatenate([jnp.cos(angles), -jnp.sin(angles)], axis=1)
    weights = jnp.where(jnp.arange(modes) == 0, 1.0, 2.0) / azimuth
    weights = jnp.concatenate([weights, weights]).astype(jnp.float32)
    inverse = forward.T * weights[:, None]
    return (forward, inverse)


def minmod(former, latter):
    return jnp.where(
        former * latter > 0, jnp.where(jnp.abs(former) < jnp.abs(latter), former, latter), 0.0
    )


def rusanov(left_state, right_state, normal):
    onehot = (jnp.arange(4) == normal).astype(left_state.dtype).reshape(4, 1, 1, 1)

    def flux_of(values):
        velocity = values[normal] / values[0]
        return (values * velocity + sound_sq * values[0] * onehot, jnp.abs(velocity))

    flux_left, speed_left = flux_of(left_state)
    flux_right, speed_right = flux_of(right_state)
    reach = jnp.maximum(speed_left, speed_right) + math.sqrt(sound_sq)
    return 0.5 * (flux_left + flux_right) - 0.5 * reach * (right_state - left_state)


def advance(padded, potential, radial_slope, centres, radial_step):
    azimuth = padded.shape[-1]
    phi_step = 2.0 * math.pi / azimuth
    step_time = courant * min(radial_step, inner_radius * phi_step)
    slopes = minmod(padded[:, 1:-1] - padded[:, :-2], padded[:, 2:] - padded[:, 1:-1])
    centre_cells = padded[:, 1:-1]
    flux_radial = rusanov(
        centre_cells[:, :-1] + 0.5 * slopes[:, :-1], centre_cells[:, 1:] - 0.5 * slopes[:, 1:], 1
    )
    interior = padded[:, 2:-2]
    phi_slopes = minmod(
        interior - jnp.roll(interior, 1, axis=3), jnp.roll(interior, -1, axis=3) - interior
    )
    flux_phi = rusanov(
        interior + 0.5 * phi_slopes, jnp.roll(interior - 0.5 * phi_slopes, -1, axis=3), 2
    )
    face_radii = jnp.concatenate(
        [centres - 0.5 * radial_step, centres[-1:] + 0.5 * radial_step]
    ).reshape(1, -1, 1, 1)
    weighted = face_radii * flux_radial
    radius = centres.reshape(1, -1, 1, 1)
    tendency = (
        -(
            (weighted[:, 1:] - weighted[:, :-1]) / radial_step
            + (flux_phi - jnp.roll(flux_phi, 1, axis=3)) / phi_step
        )
        / radius
    )
    density = interior[0]
    spin = interior[2] / density
    radius_cells = centres.reshape(-1, 1, 1)
    azimuth_slope = (jnp.roll(potential, -1, axis=2) - jnp.roll(potential, 1, axis=2)) / (
        2.0 * phi_step
    )
    force_radial = (interior[2] * spin + sound_sq * density) / radius_cells - density * radial_slope
    force_phi = -(interior[1] * spin + density * azimuth_slope) / radius_cells
    zeros = jnp.zeros_like(density)
    sources = jnp.stack([zeros, force_radial, force_phi, zeros])
    return interior + step_time * (tendency + sources)


def mend_edges(padded, width, axis_dim):
    length = padded.shape[axis_dim]
    position = lax.axis_index("row")
    last_rank = lax.axis_size("row") - 1
    low_rim = lax.slice_in_dim(padded, 0, width, axis=axis_dim)
    middle = lax.slice_in_dim(padded, width, length - width, axis=axis_dim)
    high_rim = lax.slice_in_dim(padded, length - width, length, axis=axis_dim)
    first_cell = lax.slice_in_dim(middle, 0, 1, axis=axis_dim)
    last_cell = lax.slice_in_dim(
        middle, middle.shape[axis_dim] - 1, middle.shape[axis_dim], axis=axis_dim
    )
    low_rim = jnp.where(position == 0, jnp.broadcast_to(first_cell, low_rim.shape), low_rim)
    high_rim = jnp.where(
        position == last_rank, jnp.broadcast_to(last_cell, high_rim.shape), high_rim
    )
    return jnp.concatenate([low_rim, middle, high_rim], axis=axis_dim)


def plain_body(state, green, vertical):
    radii, planes, azimuth = (state.shape[1], state.shape[2], state.shape[3])
    modes_dev, radial_all = (green.shape[0], green.shape[1])
    modes = modes_dev * lax.axis_size("row")
    radial_step = radial_span / radial_all
    forward, inverse = mode_table(azimuth, modes)
    padded_state = mend_edges(padded_2(state, (("row", 1),), 2), 2, 1)
    spectrum = jnp.dot(
        state[0].reshape(-1, azimuth),
        forward,
        precision=precise,
        preferred_element_type=jnp.float32,
    ).reshape(radii, planes, 2, modes)
    plane_start = lax.axis_index("gz") * planes
    column_all = lax.all_gather(spectrum, "gz", axis=1, tiled=True)
    own_rows = lax.dynamic_slice_in_dim(vertical, plane_start, planes, 0)
    mixed = jnp.einsum("zy,ryck->rzck", own_rows, column_all, precision=precise)
    mixed_b = mixed.astype(jnp.bfloat16)
    pot_modes = jnp.einsum(
        "mrs,skcm->rkcm",
        green,
        lax.all_to_all(mixed_b, "row", split_axis=3, concat_axis=0, tiled=True),
        preferred_element_type=jnp.float32,
    )
    pot_spec = lax.all_to_all(pot_modes, "row", split_axis=0, concat_axis=3, tiled=True)
    potential = jnp.dot(
        pot_spec.reshape(-1, 2 * modes),
        inverse,
        precision=precise,
        preferred_element_type=jnp.float32,
    ).reshape(radii, planes, azimuth)
    padded_pot = mend_edges(padded_2(potential, (("row", 0),), 1), 1, 0)
    radial_slope = (padded_pot[2:] - padded_pot[:-2]) / (2.0 * radial_step)
    offsets = (lax.axis_index("row") * radii + jnp.arange(radii, dtype=jnp.int32)).astype(
        jnp.float32
    )
    centres = inner_radius + (offsets + 0.5) * radial_step
    new_state = advance(padded_state, potential, radial_slope, centres, radial_step)
    return (new_state, potential)


LANES = 128
SUBS = 8
HALF = 4
PAIRS = ((0, 0), (0, 1), (1, 0), (0, 2), (2, 0), (1, 1))


def np_split3(values):
    high = np.asarray(values, np.float32)
    parts = []
    for _ in range(3):
        part = high.astype(jnp.bfloat16)
        parts.append(part)
        high = high - part.astype(np.float32)
    return parts


def np_tables(azimuth, modes):
    index = np.arange(azimuth)[:, None] * np.arange(modes)[None, :] % azimuth
    angles = index * (2.0 * np.pi / azimuth)
    forward = np.concatenate([np.cos(angles), -np.sin(angles)], axis=1)
    weights = np.where(np.arange(modes) == 0, 1.0, 2.0) / azimuth
    inverse = forward.T * np.concatenate([weights, weights])[:, None]
    phi_step = 2.0 * np.pi / azimuth
    turned = (np.roll(inverse, -1, 1) - np.roll(inverse, 1, 1)) / (2.0 * phi_step)
    return (forward, inverse, turned)


def forward_table(forward):
    azimuth, width = forward.shape
    tiles = azimuth // (2 * LANES)
    table = np.zeros((tiles, LANES, 2, HALF, width), jnp.bfloat16)
    blocks = forward.reshape(tiles, 2, LANES, width)
    for q, part in enumerate(np_split3(blocks)):
        table[:, :, :, q] = part.transpose(0, 2, 1, 3)
    return table.reshape(tiles * LANES, 2 * HALF * width)


def inverse_table(inverse):
    width, azimuth = inverse.shape
    tiles = azimuth // (2 * LANES)
    parts = np_split3(inverse.reshape(width, tiles, 2, LANES))
    table = np.zeros((2, LANES // width, width, tiles, LANES), jnp.bfloat16)
    for q, (_, right) in enumerate(PAIRS):
        table[:, q] = parts[right].transpose(2, 0, 1, 3)
    return table.reshape(2 * LANES, tiles * LANES)


def split(values, count):
    parts = []
    for _ in range(count):
        part = values.astype(jnp.bfloat16)
        parts.append(part)
        values = values - part.astype(jnp.float32)
    return parts


def lane_of(shape):
    return lax.broadcasted_iota(jnp.int32, shape, len(shape) - 1)


def spectrum_kernel(copies, cells_ref, table_ref, out_ref, sums_ref):
    step = pl.program_id(0)
    rows, _, _ = cells_ref.shape[1:]
    tiles = cells_ref.shape[2] // SUBS
    total = None
    for t in range(0, tiles, 2):
        cells = jnp.concatenate(
            [
                cells_ref[0, :, (t + h) * SUBS : (t + h + 1) * SUBS, :].reshape(rows * SUBS, LANES)
                for h in range(2)
            ],
            axis=1,
        )
        table = table_ref[t * LANES : (t + 2) * LANES, :]
        for part in split(cells, 2):
            term = jnp.dot(part, table, preferred_element_type=jnp.float32)
            total = term if total is None else total + term
    sums_ref[pl.ds(pl.multiple_of(step * rows * SUBS, SUBS), rows * SUBS), :] = total

    @pl.when(step == pl.num_programs(0) - 1)
    def _():
        radii = sums_ref.shape[0] // SUBS
        modes = out_ref.shape[0]
        width = 2 * modes
        lane = lane_of((radii, LANES))
        for z in range(HALF):
            former = sums_ref[pl.ds(z, radii, stride=SUBS), :]
            latter = sums_ref[pl.ds(HALF + z, radii, stride=SUBS), :]
            turned = jnp.where(lane < LANES // 2, former, latter).T
            both = turned[: LANES // 2] + turned[LANES // 2 :]
            value = both[:width] + both[width : 2 * width] + both[2 * width : 3 * width]
            for c in range(2):
                for g in range(copies):
                    out_ref[:, g, c * HALF + z, :] = value[c * modes : (c + 1) * modes]


def green_kernel(cells_ref, weights_ref, green_ref, out_ref):
    blocks = cells_ref.shape[0]
    mixed = [
        jnp.dot(
            weights_ref[...],
            cells_ref[i],
            precision=precise,
            preferred_element_type=jnp.float32,
        )
        for i in range(blocks)
    ]
    mixed = jnp.concatenate(mixed, axis=1).astype(jnp.bfloat16)
    pot = lax.dot_general(
        mixed, green_ref[0], (((1,), (1,)), ((), ())), preferred_element_type=jnp.float32
    )
    lane = lane_of((SUBS, LANES))
    pieces = [pot[:, i * LANES : (i + 1) * LANES] for i in range(blocks)]
    for i in range(blocks):
        out_ref[i, 0] = pieces[i]
        low = pieces[0] if i == 0 else pltpu.roll(pieces[i - 1], 1, 1)
        if i == blocks - 1:
            high = pltpu.roll(pieces[i], 2, 1)
        else:
            high = pltpu.roll(pieces[i + 1], 1, 1)
        out_ref[i, 1] = jnp.where(lane == 0, low, high)


def limited(former, latter):
    return jnp.maximum(jnp.minimum(former, latter), jnp.minimum(jnp.maximum(former, latter), 0.0))


def face_flux(left, right, normal):
    speed_left = left[normal] / left[0]
    speed_right = right[normal] / right[0]
    reach = jnp.maximum(jnp.abs(speed_left), jnp.abs(speed_right)) + math.sqrt(sound_sq)
    weight_left = speed_left + reach
    weight_right = speed_right - reach
    fluxes = [a * weight_left + b * weight_right for a, b in zip(left, right)]
    fluxes[normal] = fluxes[normal] + sound_sq * (left[0] + right[0])
    return fluxes


def turned_lanes(chunk, ahead):
    lane = lane_of(chunk.shape) % (LANES // 2)
    if ahead:
        return jnp.where(
            lane >= LANES // 2 - HALF,
            pltpu.roll(chunk, LANES // 2 - HALF, 1),
            pltpu.roll(chunk, LANES - HALF, 1),
        )
    return jnp.where(
        lane < HALF, pltpu.roll(chunk, LANES // 2 + HALF, 1), pltpu.roll(chunk, HALF, 1)
    )


def block_step(raw, base_rows, constants, scratch, store, fresh, prepare):
    rows, subs, radial_step, phi_step, step_time = constants
    t_ref, r_ref, g_ref, o_ref, l_ref, f_ref = scratch
    chunks = LANES // SUBS

    def bring(r):
        for f in range(4):
            both = jnp.concatenate([raw(f, 0, r), raw(f, 1, r)], axis=0).T
            t_ref[r % rows, f, SUBS : SUBS + LANES, :] = both
            t_ref[r % rows, f, SUBS + LANES :, :] = turned_lanes(both[:SUBS], True)
            t_ref[r % rows, f, :SUBS, :] = turned_lanes(both[LANES - SUBS :], False)

    def cell(f, r, q, shift=0):
        return t_ref[r % rows, f, pl.ds(SUBS + q * SUBS + shift, SUBS), :]

    def radial_face(r, q):
        part = pl.ds(q * SUBS, SUBS)
        left, right = [], []
        for f in range(4):
            here, above, far = cell(f, r, q), cell(f, r + 1, q), cell(f, r + 2, q)
            slope = limited(above - here, far - above)
            twice = above + above
            left.append(l_ref[f, part, :])
            right.append(twice - slope)
            l_ref[f, part, :] = twice + slope
        return face_flux(left, right, 1)

    @pl.when(fresh)
    def _():
        for r in range(-2, 2):
            bring(r)
        for q in range(chunks):
            part = pl.ds(q * SUBS, SUBS)
            for f in range(4):
                lower, here, above = cell(f, -2, q), cell(f, -1, q), cell(f, 0, q)
                l_ref[f, part, :] = (here + here) + limited(here - lower, above - here)
            for f, value in enumerate(radial_face(-1, q)):
                f_ref[f, part, :] = value

    prepare()
    half = lane_of((SUBS, LANES)) < LANES // 2
    for r in range(rows):
        slot = r % 2
        bring(r + 2)
        index = jnp.where(half, base_rows[0] + r, base_rows[1] + r).astype(jnp.float32)
        centre = inner_radius + (index + 0.5) * radial_step
        over = step_time / centre
        scale = over * (0.25 / radial_step)
        outer = scale * (centre + 0.5 * radial_step)
        inner = scale * (centre - 0.5 * radial_step)
        turn = over * (0.25 / phi_step)

        def edges(q):
            lefts = []
            for f in range(4):
                here = cell(f, r, q)
                slope = limited(here - cell(f, r, q, -1), cell(f, r, q, 1) - here)
                twice = here + here
                lefts.append(twice + slope)
                right = twice - slope
                r_ref[slot, f, pl.ds(q * SUBS, SUBS), :] = right
                if q == 0:
                    r_ref[slot, f, pl.ds(LANES, SUBS), :] = turned_lanes(right, True)
            return lefts

        def finish(q, fluxes):
            part = pl.ds(q * SUBS, SUBS)
            radial = radial_face(r, q)
            values = [cell(f, r, q) for f in range(4)]
            density, push, swing, _ = values
            spin = swing / density
            extra = [None, (swing * spin + sound_sq * density) * over, (push * spin) * -over, None]
            for f, value in enumerate(values):
                before = g_ref[slot, f, pl.ds(SUBS + q * SUBS - 1, SUBS), :]
                value = value + (inner * f_ref[f, part, :] - outer * radial[f])
                value = value - turn * (fluxes[f] - before)
                if extra[f] is not None:
                    value = value + extra[f]
                f_ref[f, part, :] = radial[f]
                o_ref[slot, f, part, :] = value

        lefts = edges(0)
        for q in range(chunks):
            later = edges(q + 1) if q + 1 < chunks else None
            right = [r_ref[slot, f, pl.ds(q * SUBS + 1, SUBS), :] for f in range(4)]
            fluxes = face_flux(lefts, right, 2)
            for f in range(4):
                g_ref[slot, f, pl.ds(SUBS + q * SUBS, SUBS), :] = fluxes[f]
                if q == chunks - 1:
                    g_ref[slot, f, :SUBS, :] = turned_lanes(fluxes[f], False)
            if q > 0:
                finish(q, fluxes)
            lefts = later
        finish(0, [g_ref[slot, f, SUBS : 2 * SUBS, :] for f in range(4)])
        for f in range(4):
            both = o_ref[slot, f].T
            for h in range(2):
                store(f, h, r, both[h * subs : (h + 1) * subs])


def spectral_rows(modes_ref, left_ref, radial_step, step_time):
    modes = modes_ref.shape[0]
    width = 2 * modes
    radii = LANES
    lane = lane_of((modes, LANES))
    index = (lane + lax.axis_index("row") * radii).astype(jnp.float32)
    over = step_time / (inner_radius + (index + 0.5) * radial_step)
    left_ref[...] = jnp.zeros_like(left_ref)
    for z in range(HALF):
        kinds = ([], [], [])
        for c in range(2):
            here = modes_ref[:, 0, c * HALF + z, :]
            edge = modes_ref[:, 1, c * HALF + z, :]
            above = jnp.where(
                lane == LANES - 1, pltpu.roll(edge, LANES - 2, 1), pltpu.roll(here, LANES - 1, 1)
            )
            below = jnp.where(lane == 0, edge, pltpu.roll(here, 1, 1))
            kinds[0].append(here)
            kinds[1].append((above - below) * (step_time / (2.0 * radial_step)))
            kinds[2].append(here * over)
        for kind, halves in enumerate(kinds):
            parts = [part.astype(jnp.float32) for part in split(jnp.concatenate(halves, axis=0), 3)]
            stack = [parts[left] for left, _ in PAIRS]
            stack += [jnp.zeros((LANES - len(PAIRS) * width, LANES), jnp.float32)]
            turned = jnp.concatenate(stack, axis=0).T
            for p in range(2):
                left_ref[kind, p, pl.ds(p * HALF + z, radii, stride=SUBS), :] = turned


def muscl_kernel(plan, final, *refs):
    rows, subs, radii, radial_all, start, count, done = plan
    if final:
        cells, low, high, modes_ref, pot_table, turn_table, old, out, pot_out, *refs = refs
        left_ref, pull_ref, pot_buf, late_buf, late_pot, pot_sem, late_sem, *refs = refs
    else:
        cells, out, *refs = refs
    in_buf, out_buf, in_sem, head_sem, out_sem, *scratch = refs
    azimuth = subs // HALF * LANES
    phi_step = 2.0 * math.pi / azimuth
    radial_step = radial_span / radial_all
    step_time = courant * min(radial_step, inner_radius * phi_step)
    span = radii // 2
    blocks = span // rows
    size = rows * subs
    position = lax.axis_index("row")
    last_rank = lax.axis_size("row") - 1
    tiles = subs // SUBS

    def place(n):
        return lax.rem(start + n, blocks)

    def line(row):
        return pl.multiple_of(row * subs, subs)

    def copy_in(source, f, h, row, count_rows, slot, offset, sem):
        return pltpu.make_async_copy(
            source.at[f, pl.ds(line(row), count_rows * subs), :],
            in_buf.at[slot, f, h, pl.ds(offset * subs, count_rows * subs), :],
            sem,
        )

    def fetch(n, slot):
        b = place(n)
        first = b * rows
        lowest = b == 0
        highest = b == blocks - 1
        sem = in_sem.at[slot]
        head_one = head_sem.at[0]

        for f in range(4):
            copy_in(cells, f, 0, first, rows + 2, slot, 2, sem).start()

        @pl.when(jnp.logical_not(highest))
        def _():
            for f in range(4):
                copy_in(cells, f, 1, span + first, rows + 2, slot, 2, sem).start()

        @pl.when((n == 0) | lowest)
        def _():
            for f in range(4):
                copy_in(cells, f, 1, span + first - 2, 2, slot, 0, head_one).start()

        @pl.when((n == 0) & jnp.logical_not(lowest))
        def _():
            for f in range(4):
                copy_in(cells, f, 0, first - 2, 2, slot, 0, head_one).start()

        if not final:
            return

        @pl.when(highest)
        def _():
            for f in range(4):
                copy_in(cells, f, 1, radii - rows, rows, slot, 2, sem).start()

            @pl.when(position == last_rank)
            def _():
                for f in range(4):
                    for i in range(2):
                        copy_in(cells, f, 1, radii - 1, 1, slot, 2 + rows + i, sem).start()

            @pl.when(position != last_rank)
            def _():
                for f in range(4):
                    copy_in(high, f, 1, 0, 2, slot, 2 + rows, sem).start()

        @pl.when(lowest)
        def _():
            @pl.when(position == 0)
            def _():
                for f in range(4):
                    for i in range(2):
                        copy_in(cells, f, 0, 0, 1, slot, i, head_one).start()

            @pl.when(position != 0)
            def _():
                for f in range(4):
                    copy_in(low, f, 0, 0, 2, slot, 0, head_one).start()

    def arrived(slot, fresh):
        for f in range(4):
            for h in range(2):
                copy_in(cells, f, h, 0, rows + 2, slot, 2, in_sem.at[slot]).wait()

        @pl.when(fresh)
        def _():
            for f in range(4):
                for h in range(2):
                    copy_in(cells, f, h, 0, 2, slot, 0, head_sem.at[0]).wait()

    def result(b, slot, fields, sem):
        copies = []
        for h in range(2):
            part = pl.ds(line(h * span + b * rows), size)
            for f in fields:
                copies.append(
                    pltpu.make_async_copy(
                        out_buf.at[slot, f, h, pl.ds(0, size), :], out.at[f, part, :], sem.at[slot]
                    )
                )
            if final:
                copies.append(
                    pltpu.make_async_copy(pot_buf.at[slot, h], pot_out.at[part, :], sem.at[slot])
                )
        return copies

    def late_in(n):
        copies = []
        for h in range(2):
            part = pl.ds((h * span + (1 + n) * rows) * subs, size)
            for i, (source, f) in enumerate(((cells, 0), (out, 1), (out, 2))):
                copies.append(
                    pltpu.make_async_copy(
                        source.at[f, part, :], late_buf.at[n, i, h], late_sem.at[n]
                    )
                )
        return copies

    def late_out(n):
        copies = []
        for h in range(2):
            part = pl.ds((h * span + (1 + n) * rows) * subs, size)
            for f in (1, 2):
                copies.append(
                    pltpu.make_async_copy(late_buf.at[n, f, h], out.at[f, part, :], pot_sem.at[n])
                )
            copies.append(
                pltpu.make_async_copy(late_pot.at[n, h], pot_out.at[part, :], pot_sem.at[n])
            )
        return copies

    fetch(0, 0)
    if final:
        for n in range(done):
            for copy in late_in(n):
                copy.start()
        spectral_rows(modes_ref, left_ref, radial_step, step_time)

    def spectral(b, pot_here):
        lines = [
            pl.ds((h * span + b * rows) * SUBS if isinstance(b, int) else pl.multiple_of((h * span + b * rows) * SUBS, SUBS), rows * SUBS)
            for h in range(2)
        ]

        def product(kinds, table):
            left = [
                jnp.concatenate([left_ref[kind, p, where, :] for p in range(2)], axis=1)
                for kind in kinds
                for where in lines
            ]
            left = jnp.concatenate(left, axis=0).astype(jnp.bfloat16)
            return jnp.dot(left, table[...], preferred_element_type=jnp.float32)

        both = product((0, 1), pot_table)
        turn = product((2,), turn_table)
        for h in range(2):
            for r in range(rows):
                low_line = (h * rows + r) * SUBS
                pull_line = ((2 + h) * rows + r) * SUBS
                for t in range(tiles):
                    part = pl.ds(r * subs + t * SUBS, SUBS)
                    column = slice(t * LANES, (t + 1) * LANES)
                    pot_here[h, part, :] = both[low_line : low_line + SUBS, column]
                    pull_ref[0, h, part, :] = both[pull_line : pull_line + SUBS, column]
                    pull_ref[1, h, part, :] = turn[low_line : low_line + SUBS, column]

    if final:
        for n in range(done):
            spectral(1 + n, late_pot.at[n])
            for copy in late_in(n):
                copy.wait()
            for h in range(2):
                for t in range(rows * tiles):
                    part = pl.ds(t * SUBS, SUBS)
                    density = late_buf[n, 0, h, part, :]
                    for f in (1, 2):
                        late_buf[n, f, h, part, :] = (
                            late_buf[n, f, h, part, :] - density * pull_ref[f - 1, h, part, :]
                        )
            for copy in late_out(n):
                copy.start()

    def body(n, carry):
        slot = lax.rem(n, 2)

        @pl.when(n + 1 < count)
        def _():
            fetch(n + 1, 1 - slot)

        @pl.when(n >= 2)
        def _():
            for copy in result(place(n - 2), slot, range(4), out_sem):
                copy.wait()

        b = place(n)
        fresh = (n == 0) | (b == 0)
        arrived(slot, fresh)

        def prepare():
            if final:
                spectral(b, pot_buf.at[slot])

        def raw(f, h, r):
            return in_buf[slot, f, h, pl.ds((r + 2) * subs, subs), :]

        def store(f, h, r, value):
            part = pl.ds(r * subs, subs)
            if final and f in (1, 2):
                value = value - raw(0, h, r) * pull_ref[f - 1, h, part, :]
            out_buf[slot, f, h, part, :] = value

        constants = (rows, subs, radial_step, phi_step, step_time)
        base = position * radii + b * rows
        block_step(raw, (base, base + span), constants, scratch, store, fresh, prepare)
        for copy in result(b, slot, range(4), out_sem):
            copy.start()
        return carry

    lax.fori_loop(0, count, body, 0)
    for n in range(max(count - 2, 0), count):
        for copy in result(place(n), n % 2, range(4), out_sem):
            copy.wait()
    if final:
        for n in range(done):
            for copy in late_out(n):
                copy.wait()


def vmem_limit(mebibytes):
    return pltpu.CompilerParams(vmem_limit_bytes=mebibytes * 2**20)


def muscl(operands, plan, final, shape):
    rows, subs, radii, _, _, count, done = plan
    fields = shape[0]
    size = rows * subs
    anywhere = pl.BlockSpec(memory_space=pl.ANY)
    whole = pl.BlockSpec(memory_space=pltpu.VMEM)
    carried = [
        pltpu.VMEM((2, fields, 2, (rows + 4) * subs, LANES), jnp.float32),
        pltpu.VMEM((2, fields, 2, size, LANES), jnp.float32),
        pltpu.SemaphoreType.DMA((2,)),
        pltpu.SemaphoreType.DMA((1,)),
        pltpu.SemaphoreType.DMA((2,)),
        pltpu.VMEM((rows, fields, LANES + 2 * SUBS, LANES), jnp.float32),
        pltpu.VMEM((2, fields, LANES + SUBS, LANES), jnp.float32),
        pltpu.VMEM((2, fields, LANES + SUBS, LANES), jnp.float32),
        pltpu.VMEM((2, fields, LANES, LANES), jnp.float32),
        pltpu.VMEM((fields, LANES, LANES), jnp.float32),
        pltpu.VMEM((fields, LANES, LANES), jnp.float32),
    ]
    out_shape = [jax.ShapeDtypeStruct(shape, jnp.float32)]
    if final:
        in_specs = [anywhere] * 3 + [whole] * 3 + [anywhere]
        out_shape.append(jax.ShapeDtypeStruct(shape[1:], jnp.float32))
        aliases = {6: 0}
        carried = [
            pltpu.VMEM((3, 2, radii * SUBS, LANES), jnp.float32),
            pltpu.VMEM((2, 2, size, LANES), jnp.float32),
            pltpu.VMEM((2, 2, size, LANES), jnp.float32),
            pltpu.VMEM((done, 3, 2, size, LANES), jnp.float32),
            pltpu.VMEM((done, 2, size, LANES), jnp.float32),
            pltpu.SemaphoreType.DMA((done,)),
            pltpu.SemaphoreType.DMA((done,)),
        ] + carried
    else:
        in_specs = [anywhere]
        aliases = {}
    return pl.pallas_call(
        lambda *refs: muscl_kernel(plan, final, *refs),
        name="muscl_final" if final else "muscl_early",
        in_specs=in_specs,
        out_specs=[anywhere] * len(out_shape),
        out_shape=out_shape,
        input_output_aliases=aliases,
        scratch_shapes=carried,
        compiler_params=vmem_limit(50),
        cost_estimate=pl.CostEstimate(
            flops=count * rows * subs * LANES * 3000,
            bytes_accessed=count * size * LANES * 64,
            transcendentals=0,
        ),
    )(*operands)


def fast_body(state, green, vertical):
    fields, radii, planes, azimuth = state.shape
    radial_all = green.shape[1]
    ranks, stacks = lax.axis_size("row"), lax.axis_size("gz")
    modes = green.shape[0] * ranks
    subs = azimuth // LANES * planes
    forward, inverse, turned = np_tables(azimuth, modes)
    cells = (
        state.reshape(fields, radii, planes, azimuth // LANES, LANES)
        .transpose(0, 1, 3, 2, 4)
        .reshape(fields, radii, subs, LANES)
    )
    up_ring = [(i, i + 1) for i in range(ranks - 1)]
    low = lax.ppermute(cells[:, radii - 2 :], "row", up_ring)
    high = lax.ppermute(cells[:, :2], "row", [(j, i) for i, j in up_ring])

    rows = 32
    spectrum = pl.pallas_call(
        lambda *refs: spectrum_kernel(stacks, *refs),
        name="spectrum",
        grid=(radii // rows,),
        in_specs=[
            pl.BlockSpec((1, rows, subs, LANES), lambda i: (0, i, 0, 0)),
            pl.BlockSpec((azimuth // 2, LANES), lambda i: (0, 0)),
        ],
        out_specs=pl.BlockSpec((modes, stacks, SUBS, LANES), lambda i: (0, 0, 0, 0)),
        out_shape=jax.ShapeDtypeStruct((modes, stacks, SUBS, LANES), jnp.float32),
        scratch_shapes=[pltpu.VMEM((radii * SUBS, LANES), jnp.float32)],
        compiler_params=vmem_limit(54),
        cost_estimate=pl.CostEstimate(flops=2**33, bytes_accessed=2**22, transcendentals=0),
    )(cells, forward_table(forward))

    gathered = lax.all_to_all(
        spectrum.reshape(ranks * stacks, SUBS, LANES), ("row", "gz"), 0, 0, tiled=True
    )
    own = lax.dynamic_slice_in_dim(vertical, lax.axis_index("gz") * planes, planes, 0)
    own = own.reshape(planes, stacks, planes)
    weights = jnp.einsum("cd,zgy->czgdy", jnp.eye(2, dtype=jnp.float32), own, precision=precise)
    weights = weights.reshape(SUBS, stacks * SUBS)

    pot_modes = pl.pallas_call(
        green_kernel,
        name="green",
        in_specs=[pl.BlockSpec(memory_space=pltpu.VMEM)] * 3,
        out_specs=pl.BlockSpec(memory_space=pltpu.VMEM),
        out_shape=jax.ShapeDtypeStruct((ranks, 2, SUBS, LANES), jnp.float32),
        compiler_params=vmem_limit(16),
        cost_estimate=pl.CostEstimate(flops=2**30, bytes_accessed=2**21, transcendentals=0),
    )(gathered.reshape(ranks, stacks * SUBS, LANES), weights, green)
    pot_spec = lax.all_to_all(pot_modes, "row", 0, 0, tiled=True)

    rows, early = 4, 2
    blocks = radii // 2 // rows
    flat = cells.reshape(fields, radii * subs, LANES)
    flat_low = low.reshape(fields, 2 * subs, LANES)
    flat_high = high.reshape(fields, 2 * subs, LANES)
    plan = (rows, subs, radii, radial_all, 1, early, 0)
    (partial,) = muscl([flat], plan, False, flat.shape)
    plan = (rows, subs, radii, radial_all, 1 + early, blocks - early, early)
    new_cells, potential = muscl(
        [
            flat,
            flat_low,
            flat_high,
            pot_spec,
            inverse_table(inverse),
            inverse_table(turned),
            partial,
        ],
        plan,
        True,
        flat.shape,
    )
    new_state = (
        new_cells.reshape(fields, radii, azimuth // LANES, planes, LANES)
        .transpose(0, 1, 3, 2, 4)
        .reshape(state.shape)
    )
    potential = (
        potential.reshape(radii, azimuth // LANES, planes, LANES)
        .transpose(0, 2, 1, 3)
        .reshape(state.shape[1:])
    )
    return (new_state, potential)


def body(state, green, vertical):
    _, radii, planes, azimuth = state.shape
    modes = green.shape[0] * lax.axis_size("row")
    fits = (
        planes == HALF
        and azimuth % (4 * LANES) == 0
        and radii == LANES
        and green.shape[0] == 1
        and modes == SUBS
    )
    return (fast_body if fits else plain_body)(state, green, vertical)


def solution(mesh):
    placed = (P(None, "row", "gz", None), P("row", None, None), P())
    return jax.shard_map(
        body,
        mesh=mesh,
        in_specs=placed,
        out_specs=(P(None, "row", "gz", None), P("row", "gz", None)),
        check_vma=False,
    )
```

```python
import math

import jax
import jax.numpy as jnp
import numpy as np
from jax import lax
from jax.experimental import pallas as pl
from jax.experimental.pallas import tpu as pltpu
from jax.sharding import PartitionSpec as P

sound_sq = 1.0
inner_radius = 1.0
radial_span = 4.0
courant = 0.2
precise = lax.Precision.HIGHEST


def padded_2(cells, sides, width):
    for axis, dim in sides:
        count = lax.axis_size(axis)
        ends = count - 1
        head = lax.slice_in_dim(cells, 0, width, axis=dim)
        tail = lax.slice_in_dim(cells, cells.shape[dim] - width, cells.shape[dim], axis=dim)
        cells = jnp.concatenate(
            [
                lax.ppermute(tail, axis, [(i, (i + 1) % count) for i in range(ends)]),
                cells,
                lax.ppermute(head, axis, [((i + 1) % count, i) for i in range(ends)]),
            ],
            axis=dim,
        )
    return cells


def mode_table(azimuth, modes):
    angle_index = (
        jnp.arange(azimuth, dtype=jnp.int32)[:, None]
        * jnp.arange(modes, dtype=jnp.int32)[None, :]
        % azimuth
    )
    angles = angle_index.astype(jnp.float32) * (2.0 * math.pi / azimuth)
    forward = jnp.concatenate([jnp.cos(angles), -jnp.sin(angles)], axis=1)
    weights = jnp.where(jnp.arange(modes) == 0, 1.0, 2.0) / azimuth
    weights = jnp.concatenate([weights, weights]).astype(jnp.float32)
    inverse = forward.T * weights[:, None]
    return (forward, inverse)


def minmod(former, latter):
    return jnp.where(
        former * latter > 0, jnp.where(jnp.abs(former) < jnp.abs(latter), former, latter), 0.0
    )


def rusanov(left_state, right_state, normal):
    onehot = (jnp.arange(4) == normal).astype(left_state.dtype).reshape(4, 1, 1, 1)

    def flux_of(values):
        velocity = values[normal] / values[0]
        return (values * velocity + sound_sq * values[0] * onehot, jnp.abs(velocity))

    flux_left, speed_left = flux_of(left_state)
    flux_right, speed_right = flux_of(right_state)
    reach = jnp.maximum(speed_left, speed_right) + math.sqrt(sound_sq)
    return 0.5 * (flux_left + flux_right) - 0.5 * reach * (right_state - left_state)


def advance(padded, potential, radial_slope, centres, radial_step):
    azimuth = padded.shape[-1]
    phi_step = 2.0 * math.pi / azimuth
    step_time = courant * min(radial_step, inner_radius * phi_step)
    slopes = minmod(padded[:, 1:-1] - padded[:, :-2], padded[:, 2:] - padded[:, 1:-1])
    centre_cells = padded[:, 1:-1]
    flux_radial = rusanov(
        centre_cells[:, :-1] + 0.5 * slopes[:, :-1], centre_cells[:, 1:] - 0.5 * slopes[:, 1:], 1
    )
    interior = padded[:, 2:-2]
    phi_slopes = minmod(
        interior - jnp.roll(interior, 1, axis=3), jnp.roll(interior, -1, axis=3) - interior
    )
    flux_phi = rusanov(
        interior + 0.5 * phi_slopes, jnp.roll(interior - 0.5 * phi_slopes, -1, axis=3), 2
    )
    face_radii = jnp.concatenate(
        [centres - 0.5 * radial_step, centres[-1:] + 0.5 * radial_step]
    ).reshape(1, -1, 1, 1)
    weighted = face_radii * flux_radial
    radius = centres.reshape(1, -1, 1, 1)
    tendency = (
        -(
            (weighted[:, 1:] - weighted[:, :-1]) / radial_step
            + (flux_phi - jnp.roll(flux_phi, 1, axis=3)) / phi_step
        )
        / radius
    )
    density = interior[0]
    spin = interior[2] / density
    radius_cells = centres.reshape(-1, 1, 1)
    azimuth_slope = (jnp.roll(potential, -1, axis=2) - jnp.roll(potential, 1, axis=2)) / (
        2.0 * phi_step
    )
    force_radial = (interior[2] * spin + sound_sq * density) / radius_cells - density * radial_slope
    force_phi = -(interior[1] * spin + density * azimuth_slope) / radius_cells
    zeros = jnp.zeros_like(density)
    sources = jnp.stack([zeros, force_radial, force_phi, zeros])
    return interior + step_time * (tendency + sources)


def mend_edges(padded, width, axis_dim):
    length = padded.shape[axis_dim]
    position = lax.axis_index("row")
    last_rank = lax.axis_size("row") - 1
    low_rim = lax.slice_in_dim(padded, 0, width, axis=axis_dim)
    middle = lax.slice_in_dim(padded, width, length - width, axis=axis_dim)
    high_rim = lax.slice_in_dim(padded, length - width, length, axis=axis_dim)
    first_cell = lax.slice_in_dim(middle, 0, 1, axis=axis_dim)
    last_cell = lax.slice_in_dim(
        middle, middle.shape[axis_dim] - 1, middle.shape[axis_dim], axis=axis_dim
    )
    low_rim = jnp.where(position == 0, jnp.broadcast_to(first_cell, low_rim.shape), low_rim)
    high_rim = jnp.where(
        position == last_rank, jnp.broadcast_to(last_cell, high_rim.shape), high_rim
    )
    return jnp.concatenate([low_rim, middle, high_rim], axis=axis_dim)


def plain_body(state, green, vertical):
    radii, planes, azimuth = (state.shape[1], state.shape[2], state.shape[3])
    modes_dev, radial_all = (green.shape[0], green.shape[1])
    modes = modes_dev * lax.axis_size("row")
    radial_step = radial_span / radial_all
    forward, inverse = mode_table(azimuth, modes)
    padded_state = mend_edges(padded_2(state, (("row", 1),), 2), 2, 1)
    spectrum = jnp.dot(
        state[0].reshape(-1, azimuth),
        forward,
        precision=precise,
        preferred_element_type=jnp.float32,
    ).reshape(radii, planes, 2, modes)
    plane_start = lax.axis_index("gz") * planes
    column_all = lax.all_gather(spectrum, "gz", axis=1, tiled=True)
    own_rows = lax.dynamic_slice_in_dim(vertical, plane_start, planes, 0)
    mixed = jnp.einsum("zy,ryck->rzck", own_rows, column_all, precision=precise)
    mixed_b = mixed.astype(jnp.bfloat16)
    pot_modes = jnp.einsum(
        "mrs,skcm->rkcm",
        green,
        lax.all_to_all(mixed_b, "row", split_axis=3, concat_axis=0, tiled=True),
        preferred_element_type=jnp.float32,
    )
    pot_spec = lax.all_to_all(pot_modes, "row", split_axis=0, concat_axis=3, tiled=True)
    potential = jnp.dot(
        pot_spec.reshape(-1, 2 * modes),
        inverse,
        precision=precise,
        preferred_element_type=jnp.float32,
    ).reshape(radii, planes, azimuth)
    padded_pot = mend_edges(padded_2(potential, (("row", 0),), 1), 1, 0)
    radial_slope = (padded_pot[2:] - padded_pot[:-2]) / (2.0 * radial_step)
    offsets = (lax.axis_index("row") * radii + jnp.arange(radii, dtype=jnp.int32)).astype(
        jnp.float32
    )
    centres = inner_radius + (offsets + 0.5) * radial_step
    new_state = advance(padded_state, potential, radial_slope, centres, radial_step)
    return (new_state, potential)


LANES = 128
SUBS = 8
HALF = 4
PAIRS = ((0, 0), (0, 1), (1, 0), (0, 2), (2, 0), (1, 1))


def np_split3(values):
    high = np.asarray(values, np.float32)
    parts = []
    for _ in range(3):
        part = high.astype(jnp.bfloat16)
        parts.append(part)
        high = high - part.astype(np.float32)
    return parts


def np_tables(azimuth, modes):
    index = np.arange(azimuth)[:, None] * np.arange(modes)[None, :] % azimuth
    angles = index * (2.0 * np.pi / azimuth)
    forward = np.concatenate([np.cos(angles), -np.sin(angles)], axis=1)
    weights = np.where(np.arange(modes) == 0, 1.0, 2.0) / azimuth
    inverse = forward.T * np.concatenate([weights, weights])[:, None]
    phi_step = 2.0 * np.pi / azimuth
    turned = (np.roll(inverse, -1, 1) - np.roll(inverse, 1, 1)) / (2.0 * phi_step)
    return (forward, inverse, turned)


def forward_table(forward):
    azimuth, width = forward.shape
    tiles = azimuth // (2 * LANES)
    table = np.zeros((tiles, LANES, 2, HALF, width), jnp.bfloat16)
    blocks = forward.reshape(tiles, 2, LANES, width)
    for q, part in enumerate(np_split3(blocks)):
        table[:, :, :, q] = part.transpose(0, 2, 1, 3)
    return table.reshape(tiles * LANES, 2 * HALF * width)


def inverse_table(inverse):
    width, azimuth = inverse.shape
    tiles = azimuth // (2 * LANES)
    parts = np_split3(inverse.reshape(width, tiles, 2, LANES))
    table = np.zeros((2, LANES // width, width, tiles, LANES), jnp.bfloat16)
    for q, (_, right) in enumerate(PAIRS):
        table[:, q] = parts[right].transpose(2, 0, 1, 3)
    return table.reshape(2 * LANES, tiles * LANES)


def split(values, count):
    parts = []
    for _ in range(count):
        part = values.astype(jnp.bfloat16)
        parts.append(part)
        values = values - part.astype(jnp.float32)
    return parts


def lane_of(shape):
    return lax.broadcasted_iota(jnp.int32, shape, len(shape) - 1)


def spectrum_kernel(copies, cells_ref, table_ref, out_ref, sums_ref):
    step = pl.program_id(0)
    rows, _, _ = cells_ref.shape[1:]
    tiles = cells_ref.shape[2] // SUBS
    total = None
    for t in range(0, tiles, 2):
        cells = jnp.concatenate(
            [
                cells_ref[0, :, (t + h) * SUBS : (t + h + 1) * SUBS, :].reshape(rows * SUBS, LANES)
                for h in range(2)
            ],
            axis=1,
        )
        table = table_ref[t * LANES : (t + 2) * LANES, :]
        for part in split(cells, 2):
            term = jnp.dot(part, table, preferred_element_type=jnp.float32)
            total = term if total is None else total + term
    sums_ref[pl.ds(pl.multiple_of(step * rows * SUBS, SUBS), rows * SUBS), :] = total

    @pl.when(step == pl.num_programs(0) - 1)
    def _():
        radii = sums_ref.shape[0] // SUBS
        modes = out_ref.shape[0]
        width = 2 * modes
        lane = lane_of((radii, LANES))
        for z in range(HALF):
            former = sums_ref[pl.ds(z, radii, stride=SUBS), :]
            latter = sums_ref[pl.ds(HALF + z, radii, stride=SUBS), :]
            turned = jnp.where(lane < LANES // 2, former, latter).T
            both = turned[: LANES // 2] + turned[LANES // 2 :]
            value = both[:width] + both[width : 2 * width] + both[2 * width : 3 * width]
            for c in range(2):
                for g in range(copies):
                    out_ref[:, g, c * HALF + z, :] = value[c * modes : (c + 1) * modes]


def green_kernel(cells_ref, weights_ref, green_ref, out_ref):
    blocks = cells_ref.shape[0]
    mixed = [
        jnp.dot(
            weights_ref[...],
            cells_ref[i],
            precision=precise,
            preferred_element_type=jnp.float32,
        )
        for i in range(blocks)
    ]
    mixed = jnp.concatenate(mixed, axis=1).astype(jnp.bfloat16)
    pot = lax.dot_general(
        mixed, green_ref[0], (((1,), (1,)), ((), ())), preferred_element_type=jnp.float32
    )
    lane = lane_of((SUBS, LANES))
    pieces = [pot[:, i * LANES : (i + 1) * LANES] for i in range(blocks)]
    for i in range(blocks):
        out_ref[i, 0] = pieces[i]
        low = pieces[0] if i == 0 else pltpu.roll(pieces[i - 1], 1, 1)
        if i == blocks - 1:
            high = pltpu.roll(pieces[i], 2, 1)
        else:
            high = pltpu.roll(pieces[i + 1], 1, 1)
        out_ref[i, 1] = jnp.where(lane == 0, low, high)


def limited(former, latter):
    return jnp.maximum(jnp.minimum(former, latter), jnp.minimum(jnp.maximum(former, latter), 0.0))


def face_flux(left, right, normal):
    speed_left = left[normal] / left[0]
    speed_right = right[normal] / right[0]
    reach = jnp.maximum(jnp.abs(speed_left), jnp.abs(speed_right)) + math.sqrt(sound_sq)
    weight_left = speed_left + reach
    weight_right = speed_right - reach
    fluxes = [a * weight_left + b * weight_right for a, b in zip(left, right)]
    fluxes[normal] = fluxes[normal] + sound_sq * (left[0] + right[0])
    return fluxes


def turned_lanes(chunk, ahead):
    lane = lane_of(chunk.shape) % (LANES // 2)
    if ahead:
        return jnp.where(
            lane >= LANES // 2 - HALF,
            pltpu.roll(chunk, LANES // 2 - HALF, 1),
            pltpu.roll(chunk, LANES - HALF, 1),
        )
    return jnp.where(
        lane < HALF, pltpu.roll(chunk, LANES // 2 + HALF, 1), pltpu.roll(chunk, HALF, 1)
    )


def block_step(raw, base_rows, constants, scratch, store, fresh, prepare):
    rows, subs, radial_step, phi_step, step_time = constants
    t_ref, r_ref, g_ref, o_ref, l_ref, f_ref, s_ref = scratch
    chunks = LANES // SUBS

    def bring(r):
        for f in range(4):
            both = jnp.concatenate([raw(f, 0, r), raw(f, 1, r)], axis=0).T
            t_ref[r % rows, f, SUBS : SUBS + LANES, :] = both
            t_ref[r % rows, f, SUBS + LANES :, :] = turned_lanes(both[:SUBS], True)
            t_ref[r % rows, f, :SUBS, :] = turned_lanes(both[LANES - SUBS :], False)

    def cell(f, r, q, shift=0):
        return t_ref[r % rows, f, pl.ds(SUBS + q * SUBS + shift, SUBS), :]

    def radial_face(r, q):
        part = pl.ds(q * SUBS, SUBS)
        left, right = [], []
        for f in range(4):
            above = cell(f, r + 1, q)
            ahead = cell(f, r + 2, q) - above
            slope = limited(s_ref[f, part, :], ahead)
            s_ref[f, part, :] = ahead
            twice = above + above
            left.append(l_ref[f, part, :])
            right.append(twice - slope)
            l_ref[f, part, :] = twice + slope
        return face_flux(left, right, 1)

    half = lane_of((SUBS, LANES)) < LANES // 2

    @pl.when(fresh)
    def _():
        lowest = jnp.where(half, base_rows[0], base_rows[1]).astype(jnp.float32)
        first_weight = (inner_radius + lowest * radial_step) * (phi_step / radial_step)
        for r in range(-2, 2):
            bring(r)
        for q in range(chunks):
            part = pl.ds(q * SUBS, SUBS)
            for f in range(4):
                lower, here, above = cell(f, -2, q), cell(f, -1, q), cell(f, 0, q)
                l_ref[f, part, :] = (here + here) + limited(here - lower, above - here)
                s_ref[f, part, :] = above - here
            for f, value in enumerate(radial_face(-1, q)):
                f_ref[f, part, :] = value * first_weight

    prepare()
    for r in range(rows):
        slot = r % 2
        bring(r + 2)
        index = jnp.where(half, base_rows[0] + r, base_rows[1] + r).astype(jnp.float32)
        centre = inner_radius + (index + 0.5) * radial_step
        over = step_time / centre
        turn = over * (0.25 / phi_step)
        weight = (centre + 0.5 * radial_step) * (phi_step / radial_step)

        def edges(q):
            lefts = []
            for f in range(4):
                here = cell(f, r, q)
                slope = limited(here - cell(f, r, q, -1), cell(f, r, q, 1) - here)
                twice = here + here
                lefts.append(twice + slope)
                right = twice - slope
                r_ref[slot, f, pl.ds(q * SUBS, SUBS), :] = right
                if q == 0:
                    r_ref[slot, f, pl.ds(LANES, SUBS), :] = turned_lanes(right, True)
            return lefts

        def finish(q, fluxes):
            part = pl.ds(q * SUBS, SUBS)
            radial = radial_face(r, q)
            values = [cell(f, r, q) for f in range(4)]
            density, push, swing, _ = values
            spin = swing / density
            spin = spin * (4.0 * phi_step)
            extra = [None, swing * spin + density * (4.0 * phi_step * sound_sq), push * -spin, None]
            for f, value in enumerate(values):
                before = g_ref[slot, f, pl.ds(SUBS + q * SUBS - 1, SUBS), :]
                face = weight * radial[f]
                change = (f_ref[f, part, :] - face) + (before - fluxes[f])
                if extra[f] is not None:
                    change = change + extra[f]
                value = value + turn * change
                f_ref[f, part, :] = face
                o_ref[slot, f, part, :] = value

        lefts = edges(0)
        for q in range(chunks):
            later = edges(q + 1) if q + 1 < chunks else None
            right = [r_ref[slot, f, pl.ds(q * SUBS + 1, SUBS), :] for f in range(4)]
            fluxes = face_flux(lefts, right, 2)
            for f in range(4):
                g_ref[slot, f, pl.ds(SUBS + q * SUBS, SUBS), :] = fluxes[f]
                if q == chunks - 1:
                    g_ref[slot, f, :SUBS, :] = turned_lanes(fluxes[f], False)
            if q > 0:
                finish(q, fluxes)
            lefts = later
        finish(0, [g_ref[slot, f, SUBS : 2 * SUBS, :] for f in range(4)])
        for f in range(4):
            both = o_ref[slot, f].T
            for h in range(2):
                store(f, h, r, both[h * subs : (h + 1) * subs])


def spectral_rows(modes_ref, left_ref, radial_step, step_time):
    modes = modes_ref.shape[0]
    width = 2 * modes
    radii = LANES
    lane = lane_of((modes, LANES))
    index = (lane + lax.axis_index("row") * radii).astype(jnp.float32)
    over = step_time / (inner_radius + (index + 0.5) * radial_step)
    left_ref[...] = jnp.zeros_like(left_ref)
    for z in range(HALF):
        kinds = ([], [], [])
        for c in range(2):
            here = modes_ref[:, 0, c * HALF + z, :]
            edge = modes_ref[:, 1, c * HALF + z, :]
            above = jnp.where(
                lane == LANES - 1, pltpu.roll(edge, LANES - 2, 1), pltpu.roll(here, LANES - 1, 1)
            )
            below = jnp.where(lane == 0, edge, pltpu.roll(here, 1, 1))
            kinds[0].append(here)
            kinds[1].append((above - below) * (step_time / (2.0 * radial_step)))
            kinds[2].append(here * over)
        for kind, halves in enumerate(kinds):
            parts = [part.astype(jnp.float32) for part in split(jnp.concatenate(halves, axis=0), 3)]
            stack = [parts[left] for left, _ in PAIRS]
            stack += [jnp.zeros((LANES - len(PAIRS) * width, LANES), jnp.float32)]
            turned = jnp.concatenate(stack, axis=0).T
            for p in range(2):
                left_ref[kind, p, pl.ds(p * HALF + z, radii, stride=SUBS), :] = turned


def muscl_kernel(plan, final, *refs):
    rows, subs, radii, radial_all, start, count, done = plan
    if final:
        cells, low, high, modes_ref, pot_table, turn_table, old, out, pot_out, *refs = refs
        left_ref, pull_ref, pot_buf, late_buf, late_pot, pot_sem, late_sem, *refs = refs
    else:
        cells, out, *refs = refs
    in_buf, out_buf, in_sem, head_sem, out_sem, *scratch = refs
    azimuth = subs // HALF * LANES
    phi_step = 2.0 * math.pi / azimuth
    radial_step = radial_span / radial_all
    step_time = courant * min(radial_step, inner_radius * phi_step)
    span = radii // 2
    blocks = span // rows
    size = rows * subs
    position = lax.axis_index("row")
    last_rank = lax.axis_size("row") - 1
    tiles = subs // SUBS

    def place(n):
        return lax.rem(start + n, blocks)

    def line(row):
        return pl.multiple_of(row * subs, subs)

    def copy_in(source, f, h, row, count_rows, slot, offset, sem):
        return pltpu.make_async_copy(
            source.at[f, pl.ds(line(row), count_rows * subs), :],
            in_buf.at[slot, f, h, pl.ds(offset * subs, count_rows * subs), :],
            sem,
        )

    def fetch(n, slot):
        b = place(n)
        first = b * rows
        lowest = b == 0
        highest = b == blocks - 1
        sem = in_sem.at[slot]
        head_one = head_sem.at[0]

        for f in range(4):
            copy_in(cells, f, 0, first, rows + 2, slot, 2, sem).start()

        @pl.when(jnp.logical_not(highest))
        def _():
            for f in range(4):
                copy_in(cells, f, 1, span + first, rows + 2, slot, 2, sem).start()

        @pl.when((n == 0) | lowest)
        def _():
            for f in range(4):
                copy_in(cells, f, 1, span + first - 2, 2, slot, 0, head_one).start()

        @pl.when((n == 0) & jnp.logical_not(lowest))
        def _():
            for f in range(4):
                copy_in(cells, f, 0, first - 2, 2, slot, 0, head_one).start()

        if not final:
            return

        @pl.when(highest)
        def _():
            for f in range(4):
                copy_in(cells, f, 1, radii - rows, rows, slot, 2, sem).start()

            @pl.when(position == last_rank)
            def _():
                for f in range(4):
                    for i in range(2):
                        copy_in(cells, f, 1, radii - 1, 1, slot, 2 + rows + i, sem).start()

            @pl.when(position != last_rank)
            def _():
                for f in range(4):
                    copy_in(high, f, 1, 0, 2, slot, 2 + rows, sem).start()

        @pl.when(lowest)
        def _():
            @pl.when(position == 0)
            def _():
                for f in range(4):
                    for i in range(2):
                        copy_in(cells, f, 0, 0, 1, slot, i, head_one).start()

            @pl.when(position != 0)
            def _():
                for f in range(4):
                    copy_in(low, f, 0, 0, 2, slot, 0, head_one).start()

    def arrived(slot, fresh):
        for f in range(4):
            for h in range(2):
                copy_in(cells, f, h, 0, rows + 2, slot, 2, in_sem.at[slot]).wait()

        @pl.when(fresh)
        def _():
            for f in range(4):
                for h in range(2):
                    copy_in(cells, f, h, 0, 2, slot, 0, head_sem.at[0]).wait()

    def result(b, slot, fields, sem):
        copies = []
        for h in range(2):
            part = pl.ds(line(h * span + b * rows), size)
            for f in fields:
                copies.append(
                    pltpu.make_async_copy(
                        out_buf.at[slot, f, h, pl.ds(0, size), :], out.at[f, part, :], sem.at[slot]
                    )
                )
            if final:
                copies.append(
                    pltpu.make_async_copy(pot_buf.at[slot, h], pot_out.at[part, :], sem.at[slot])
                )
        return copies

    def late_in(n):
        copies = []
        for h in range(2):
            part = pl.ds((h * span + (1 + n) * rows) * subs, size)
            for i, (source, f) in enumerate(((cells, 0), (out, 1), (out, 2))):
                copies.append(
                    pltpu.make_async_copy(
                        source.at[f, part, :], late_buf.at[n, i, h], late_sem.at[n]
                    )
                )
        return copies

    def late_out(n):
        copies = []
        for h in range(2):
            part = pl.ds((h * span + (1 + n) * rows) * subs, size)
            for f in (1, 2):
                copies.append(
                    pltpu.make_async_copy(late_buf.at[n, f, h], out.at[f, part, :], pot_sem.at[n])
                )
            copies.append(
                pltpu.make_async_copy(late_pot.at[n, h], pot_out.at[part, :], pot_sem.at[n])
            )
        return copies

    fetch(0, 0)
    if final:
        for n in range(done):
            for copy in late_in(n):
                copy.start()
        spectral_rows(modes_ref, left_ref, radial_step, step_time)

    def spectral(b, pot_here):
        lines = [
            pl.ds((h * span + b * rows) * SUBS if isinstance(b, int) else pl.multiple_of((h * span + b * rows) * SUBS, SUBS), rows * SUBS)
            for h in range(2)
        ]

        def product(kinds, table):
            left = [
                jnp.concatenate([left_ref[kind, p, where, :] for p in range(2)], axis=1)
                for kind in kinds
                for where in lines
            ]
            left = jnp.concatenate(left, axis=0).astype(jnp.bfloat16)
            return jnp.dot(left, table[...], preferred_element_type=jnp.float32)

        both = product((0, 1), pot_table)
        turn = product((2,), turn_table)
        for h in range(2):
            for r in range(rows):
                low_line = (h * rows + r) * SUBS
                pull_line = ((2 + h) * rows + r) * SUBS
                for t in range(tiles):
                    part = pl.ds(r * subs + t * SUBS, SUBS)
                    column = slice(t * LANES, (t + 1) * LANES)
                    pot_here[h, part, :] = both[low_line : low_line + SUBS, column]
                    pull_ref[0, h, part, :] = both[pull_line : pull_line + SUBS, column]
                    pull_ref[1, h, part, :] = turn[low_line : low_line + SUBS, column]

    if final:
        for n in range(done):
            spectral(1 + n, late_pot.at[n])
            for copy in late_in(n):
                copy.wait()
            for h in range(2):
                for t in range(rows * tiles):
                    part = pl.ds(t * SUBS, SUBS)
                    density = late_buf[n, 0, h, part, :]
                    for f in (1, 2):
                        late_buf[n, f, h, part, :] = (
                            late_buf[n, f, h, part, :] - density * pull_ref[f - 1, h, part, :]
                        )
            for copy in late_out(n):
                copy.start()

    def body(n, carry):
        slot = lax.rem(n, 2)

        @pl.when(n + 1 < count)
        def _():
            fetch(n + 1, 1 - slot)

        @pl.when(n >= 2)
        def _():
            for copy in result(place(n - 2), slot, range(4), out_sem):
                copy.wait()

        b = place(n)
        fresh = (n == 0) | (b == 0)
        arrived(slot, fresh)

        def prepare():
            if final:
                spectral(b, pot_buf.at[slot])

        def raw(f, h, r):
            return in_buf[slot, f, h, pl.ds((r + 2) * subs, subs), :]

        def store(f, h, r, value):
            part = pl.ds(r * subs, subs)
            if final and f in (1, 2):
                value = value - raw(0, h, r) * pull_ref[f - 1, h, part, :]
            out_buf[slot, f, h, part, :] = value

        constants = (rows, subs, radial_step, phi_step, step_time)
        base = position * radii + b * rows
        block_step(raw, (base, base + span), constants, scratch, store, fresh, prepare)
        for copy in result(b, slot, range(4), out_sem):
            copy.start()
        return carry

    lax.fori_loop(0, count, body, 0)
    for n in range(max(count - 2, 0), count):
        for copy in result(place(n), n % 2, range(4), out_sem):
            copy.wait()
    if final:
        for n in range(done):
            for copy in late_out(n):
                copy.wait()


def vmem_limit(mebibytes):
    return pltpu.CompilerParams(vmem_limit_bytes=mebibytes * 2**20)


def muscl(operands, plan, final, shape):
    rows, subs, radii, _, _, count, done = plan
    fields = shape[0]
    size = rows * subs
    anywhere = pl.BlockSpec(memory_space=pl.ANY)
    whole = pl.BlockSpec(memory_space=pltpu.VMEM)
    carried = [
        pltpu.VMEM((2, fields, 2, (rows + 4) * subs, LANES), jnp.float32),
        pltpu.VMEM((2, fields, 2, size, LANES), jnp.float32),
        pltpu.SemaphoreType.DMA((2,)),
        pltpu.SemaphoreType.DMA((1,)),
        pltpu.SemaphoreType.DMA((2,)),
        pltpu.VMEM((rows, fields, LANES + 2 * SUBS, LANES), jnp.float32),
        pltpu.VMEM((2, fields, LANES + SUBS, LANES), jnp.float32),
        pltpu.VMEM((2, fields, LANES + SUBS, LANES), jnp.float32),
        pltpu.VMEM((2, fields, LANES, LANES), jnp.float32),
        pltpu.VMEM((fields, LANES, LANES), jnp.float32),
        pltpu.VMEM((fields, LANES, LANES), jnp.float32),
        pltpu.VMEM((fields, LANES, LANES), jnp.float32),
    ]
    out_shape = [jax.ShapeDtypeStruct(shape, jnp.float32)]
    if final:
        in_specs = [anywhere] * 3 + [whole] * 3 + [anywhere]
        out_shape.append(jax.ShapeDtypeStruct(shape[1:], jnp.float32))
        aliases = {6: 0}
        carried = [
            pltpu.VMEM((3, 2, radii * SUBS, LANES), jnp.float32),
            pltpu.VMEM((2, 2, size, LANES), jnp.float32),
            pltpu.VMEM((2, 2, size, LANES), jnp.float32),
            pltpu.VMEM((done, 3, 2, size, LANES), jnp.float32),
            pltpu.VMEM((done, 2, size, LANES), jnp.float32),
            pltpu.SemaphoreType.DMA((done,)),
            pltpu.SemaphoreType.DMA((done,)),
        ] + carried
    else:
        in_specs = [anywhere]
        aliases = {}
    return pl.pallas_call(
        lambda *refs: muscl_kernel(plan, final, *refs),
        name="muscl_final" if final else "muscl_early",
        in_specs=in_specs,
        out_specs=[anywhere] * len(out_shape),
        out_shape=out_shape,
        input_output_aliases=aliases,
        scratch_shapes=carried,
        compiler_params=vmem_limit(50),
        cost_estimate=pl.CostEstimate(
            flops=count * rows * subs * LANES * 3000,
            bytes_accessed=count * size * LANES * 64,
            transcendentals=0,
        ),
    )(*operands)


def fast_body(state, green, vertical):
    fields, radii, planes, azimuth = state.shape
    radial_all = green.shape[1]
    ranks, stacks = lax.axis_size("row"), lax.axis_size("gz")
    modes = green.shape[0] * ranks
    subs = azimuth // LANES * planes
    forward, inverse, turned = np_tables(azimuth, modes)
    cells = (
        state.reshape(fields, radii, planes, azimuth // LANES, LANES)
        .transpose(0, 1, 3, 2, 4)
        .reshape(fields, radii, subs, LANES)
    )
    up_ring = [(i, i + 1) for i in range(ranks - 1)]
    low = lax.ppermute(cells[:, radii - 2 :], "row", up_ring)
    high = lax.ppermute(cells[:, :2], "row", [(j, i) for i, j in up_ring])

    rows = 32
    spectrum = pl.pallas_call(
        lambda *refs: spectrum_kernel(stacks, *refs),
        name="spectrum",
        grid=(radii // rows,),
        in_specs=[
            pl.BlockSpec((1, rows, subs, LANES), lambda i: (0, i, 0, 0)),
            pl.BlockSpec((azimuth // 2, LANES), lambda i: (0, 0)),
        ],
        out_specs=pl.BlockSpec((modes, stacks, SUBS, LANES), lambda i: (0, 0, 0, 0)),
        out_shape=jax.ShapeDtypeStruct((modes, stacks, SUBS, LANES), jnp.float32),
        scratch_shapes=[pltpu.VMEM((radii * SUBS, LANES), jnp.float32)],
        compiler_params=vmem_limit(54),
        cost_estimate=pl.CostEstimate(flops=2**33, bytes_accessed=2**22, transcendentals=0),
    )(cells, forward_table(forward))

    gathered = lax.all_to_all(
        spectrum.reshape(ranks * stacks, SUBS, LANES), ("row", "gz"), 0, 0, tiled=True
    )
    own = lax.dynamic_slice_in_dim(vertical, lax.axis_index("gz") * planes, planes, 0)
    own = own.reshape(planes, stacks, planes)
    weights = jnp.einsum("cd,zgy->czgdy", jnp.eye(2, dtype=jnp.float32), own, precision=precise)
    weights = weights.reshape(SUBS, stacks * SUBS)

    pot_modes = pl.pallas_call(
        green_kernel,
        name="green",
        in_specs=[pl.BlockSpec(memory_space=pltpu.VMEM)] * 3,
        out_specs=pl.BlockSpec(memory_space=pltpu.VMEM),
        out_shape=jax.ShapeDtypeStruct((ranks, 2, SUBS, LANES), jnp.float32),
        compiler_params=vmem_limit(16),
        cost_estimate=pl.CostEstimate(flops=2**30, bytes_accessed=2**21, transcendentals=0),
    )(gathered.reshape(ranks, stacks * SUBS, LANES), weights, green)
    pot_spec = lax.all_to_all(pot_modes, "row", 0, 0, tiled=True)

    rows, early = 4, 2
    blocks = radii // 2 // rows
    flat = cells.reshape(fields, radii * subs, LANES)
    flat_low = low.reshape(fields, 2 * subs, LANES)
    flat_high = high.reshape(fields, 2 * subs, LANES)
    plan = (rows, subs, radii, radial_all, 1, early, 0)
    (partial,) = muscl([flat], plan, False, flat.shape)
    plan = (rows, subs, radii, radial_all, 1 + early, blocks - early, early)
    new_cells, potential = muscl(
        [
            flat,
            flat_low,
            flat_high,
            pot_spec,
            inverse_table(inverse),
            inverse_table(turned),
            partial,
        ],
        plan,
        True,
        flat.shape,
    )
    new_state = (
        new_cells.reshape(fields, radii, azimuth // LANES, planes, LANES)
        .transpose(0, 1, 3, 2, 4)
        .reshape(state.shape)
    )
    potential = (
        potential.reshape(radii, azimuth // LANES, planes, LANES)
        .transpose(0, 2, 1, 3)
        .reshape(state.shape[1:])
    )
    return (new_state, potential)


def body(state, green, vertical):
    _, radii, planes, azimuth = state.shape
    modes = green.shape[0] * lax.axis_size("row")
    fits = (
        planes == HALF
        and azimuth % (4 * LANES) == 0
        and radii == LANES
        and green.shape[0] == 1
        and modes == SUBS
    )
    return (fast_body if fits else plain_body)(state, green, vertical)


def solution(mesh):
    placed = (P(None, "row", "gz", None), P("row", None, None), P())
    return jax.shard_map(
        body,
        mesh=mesh,
        in_specs=placed,
        out_specs=(P(None, "row", "gz", None), P("row", "gz", None)),
        check_vma=False,
    )
```
